32 devices in a mesh: dp: 1 (over z), tp: 4 (over y), cp: 8 (over x, core).
Axes of the slice: x: 4, y: 4, z: 1, core: 2. Of those that a mesh axis runs over, the one named last changes fastest.
The devices are a block of a 4x4x8 slice.
Arguments:
- x_in: bfloat16 [1024, 4096], P(('dp', 'cp', 'tp'))
- w_query: bfloat16 [4096, 32, 128], P(None, 'tp')
- w_key: bfloat16 [4096, 32, 128], P(None, 'tp')
- w_value: bfloat16 [4096, 32, 128], P(None, 'tp')
- w_out: bfloat16 [32, 128, 4096], P('tp')
- d_out: bfloat16 [1024, 4096], P(('dp', 'cp', 'tp'))
Outputs:
- output 1: bfloat16 [1024, 4096], P(('dp', 'cp', 'tp'))
- output 2: bfloat16 [1024, 4096], P(('dp', 'cp', 'tp'))
- output 3: bfloat16 [8, 4096, 32, 128], P(('dp', 'cp'), None, 'tp')
- output 4: bfloat16 [8, 4096, 32, 128], P(('dp', 'cp'), None, 'tp')
- output 5: bfloat16 [8, 4096, 32, 128], P(('dp', 'cp'), None, 'tp')
- output 6: bfloat16 [8, 32, 128, 4096], P(('dp', 'cp'), 'tp')
All inputs are finite; a program needn't handle non-finite values.
Results may differ from the reference program's by a relative error of at most 0.0102951.
Values are sent between devices in bfloat16 or wider.
A program may use at most 768 MiB of HBM per device.

```python
import math
import jax
import jax.numpy as jnp
from jax import lax

MODEL_DIM = 4096
NUM_HEADS = 32
NUM_KV_HEADS = 32
HEAD_DIM = 128
SEQ_LEN = 1024
SEQ_SHARDS = 8
QUERY_BLOCK = 32


def setup_inputs(seed: int = 0, part: int = 0) -> dict:
    shared_keys = jax.random.split(jax.random.key(seed), 4)
    part_keys = jax.random.split(jax.random.fold_in(jax.random.key(seed), part), 2)
    logit_gain = 1.6
    in_scale = 1.0 / math.sqrt(MODEL_DIM)
    x_in = jax.random.normal(part_keys[0], (SEQ_LEN, MODEL_DIM), jnp.float32)
    w_query = jax.random.normal(shared_keys[0], (MODEL_DIM, NUM_HEADS, HEAD_DIM), jnp.float32) * (logit_gain * in_scale)
    w_key = jax.random.normal(shared_keys[1], (MODEL_DIM, NUM_KV_HEADS, HEAD_DIM), jnp.float32) * (logit_gain * in_scale)
    w_value = jax.random.normal(shared_keys[2], (MODEL_DIM, NUM_KV_HEADS, HEAD_DIM), jnp.float32) * in_scale
    w_out = jax.random.normal(shared_keys[3], (NUM_HEADS, HEAD_DIM, MODEL_DIM), jnp.float32) / math.sqrt(NUM_HEADS * HEAD_DIM)
    d_out = jax.random.normal(part_keys[1], (SEQ_LEN, MODEL_DIM), jnp.float32)
    return {"x_in": x_in.astype(jnp.bfloat16), "w_query": w_query.astype(jnp.bfloat16), "w_key": w_key.astype(jnp.bfloat16), "w_value": w_value.astype(jnp.bfloat16), "w_out": w_out.astype(jnp.bfloat16), "d_out": d_out.astype(jnp.bfloat16)}


def stored_positions():
    half_rows = SEQ_LEN // (2 * SEQ_SHARDS)
    row_ids = jnp.arange(SEQ_LEN, dtype=jnp.int32)
    shard_id = row_ids // (2 * half_rows)
    within = row_ids % (2 * half_rows)
    return jnp.where(within < half_rows, shard_id * half_rows + within, (2 * SEQ_SHARDS - 1 - shard_id) * half_rows + within - half_rows)


def reference(x_in, w_query, w_key, w_value, w_out, d_out):
    groups = NUM_HEADS // NUM_KV_HEADS
    attn_scale = 1.0 / math.sqrt(HEAD_DIM)
    n_blocks = SEQ_LEN // QUERY_BLOCK
    shard_rows = SEQ_LEN // SEQ_SHARDS
    q_cols = NUM_HEADS * HEAD_DIM
    kv_cols = NUM_KV_HEADS * HEAD_DIM
    wq_flat = w_query.reshape(MODEL_DIM, q_cols)
    wk_flat = w_key.reshape(MODEL_DIM, kv_cols)
    wv_flat = w_value.reshape(MODEL_DIM, kv_cols)
    wo_flat = w_out.reshape(q_cols, MODEL_DIM)
    q_flat = jnp.dot(x_in, wq_flat, preferred_element_type=jnp.float32).astype(jnp.bfloat16)
    k_flat = jnp.dot(x_in, wk_flat, preferred_element_type=jnp.float32).astype(jnp.bfloat16)
    v_flat = jnp.dot(x_in, wv_flat, preferred_element_type=jnp.float32).astype(jnp.bfloat16)
    positions = stored_positions()
    k_heads = k_flat.reshape(SEQ_LEN, NUM_KV_HEADS, HEAD_DIM).astype(jnp.float32)
    v_heads = v_flat.reshape(SEQ_LEN, NUM_KV_HEADS, HEAD_DIM).astype(jnp.float32)
    q_blocks = q_flat.reshape(n_blocks, QUERY_BLOCK, NUM_KV_HEADS, groups, HEAD_DIM)
    pos_blocks = positions.reshape(n_blocks, QUERY_BLOCK)

    def block_scores(q_blk, pos_blk):
        scores = jnp.einsum("qhgd,khd->qhgk", q_blk.astype(jnp.float32), k_heads) * attn_scale
        visible = pos_blk[:, None, None, None] >= positions[None, None, None, :]
        return jnp.where(visible, scores, -jnp.inf)

    def forward_block(block_in):
        q_blk, pos_blk = block_in
        scores = block_scores(q_blk, pos_blk)
        row_max = jnp.max(scores, axis=-1)
        prob_mat = jnp.exp(scores - row_max[..., None])
        row_sum = jnp.sum(prob_mat, axis=-1)
        pv_sum = jnp.einsum("qhgk,khd->qhgd", prob_mat.astype(jnp.bfloat16).astype(jnp.float32), v_heads)
        out_blk = (pv_sum / row_sum[..., None]).astype(jnp.bfloat16)
        return out_blk, row_max + jnp.log(row_sum)

    o_blocks, lse_blocks = lax.map(forward_block, (q_blocks, pos_blocks))
    o_flat = o_blocks.reshape(SEQ_LEN, q_cols)
    y_out = jnp.dot(o_flat, wo_flat, preferred_element_type=jnp.float32).astype(jnp.bfloat16)

    do_flat = jnp.dot(d_out, wo_flat.T, preferred_element_type=jnp.float32).astype(jnp.bfloat16)
    do_blocks = do_flat.reshape(n_blocks, QUERY_BLOCK, NUM_KV_HEADS, groups, HEAD_DIM)
    dot_blocks = jnp.sum(do_blocks.astype(jnp.float32) * o_blocks.astype(jnp.float32), axis=-1)

    def backward_block(grad_carry, block_in):
        dk_acc, dv_acc = grad_carry
        q_blk, pos_blk, lse_blk, do_blk, dot_blk = block_in
        scores = block_scores(q_blk, pos_blk)
        prob_mat = jnp.exp(scores - lse_blk[..., None])
        do_wide = do_blk.astype(jnp.float32)
        d_probs = jnp.einsum("qhgd,khd->qhgk", do_wide, v_heads)
        d_scores = (prob_mat * (d_probs - dot_blk[..., None])).astype(jnp.bfloat16).astype(jnp.float32)
        dv_acc = dv_acc + jnp.einsum("qhgk,qhgd->khd", prob_mat.astype(jnp.bfloat16).astype(jnp.float32), do_wide)
        dk_acc = dk_acc + jnp.einsum("qhgk,qhgd->khd", d_scores, q_blk.astype(jnp.float32)) * attn_scale
        dq_blk = jnp.einsum("qhgk,khd->qhgd", d_scores, k_heads) * attn_scale
        return (dk_acc, dv_acc), dq_blk.astype(jnp.bfloat16)

    zero_kv = jnp.zeros((SEQ_LEN, NUM_KV_HEADS, HEAD_DIM), jnp.float32)
    grad_kv, dq_blocks = lax.scan(backward_block, (zero_kv, zero_kv), (q_blocks, pos_blocks, lse_blocks, do_blocks, dot_blocks))
    dq_flat = dq_blocks.reshape(SEQ_LEN, q_cols)
    dk_flat = grad_kv[0].astype(jnp.bfloat16).reshape(SEQ_LEN, kv_cols)
    dv_flat = grad_kv[1].astype(jnp.bfloat16).reshape(SEQ_LEN, kv_cols)
    dx_sum = (jnp.dot(dq_flat, wq_flat.T, preferred_element_type=jnp.float32)
              + jnp.dot(dk_flat, wk_flat.T, preferred_element_type=jnp.float32)
              + jnp.dot(dv_flat, wv_flat.T, preferred_element_type=jnp.float32))
    grad_x = dx_sum.astype(jnp.bfloat16)
    x_shards = x_in.reshape(SEQ_SHARDS, shard_rows, MODEL_DIM).astype(jnp.float32)
    grad_wq = jnp.einsum("rsm,rsc->rmc", x_shards, dq_flat.reshape(SEQ_SHARDS, shard_rows, q_cols).astype(jnp.float32)).astype(jnp.bfloat16).reshape(SEQ_SHARDS, MODEL_DIM, NUM_HEADS, HEAD_DIM)
    grad_wk = jnp.einsum("rsm,rsc->rmc", x_shards, dk_flat.reshape(SEQ_SHARDS, shard_rows, kv_cols).astype(jnp.float32)).astype(jnp.bfloat16).reshape(SEQ_SHARDS, MODEL_DIM, NUM_KV_HEADS, HEAD_DIM)
    grad_wv = jnp.einsum("rsm,rsc->rmc", x_shards, dv_flat.reshape(SEQ_SHARDS, shard_rows, kv_cols).astype(jnp.float32)).astype(jnp.bfloat16).reshape(SEQ_SHARDS, MODEL_DIM, NUM_KV_HEADS, HEAD_DIM)
    grad_wo = jnp.einsum("rsc,rsm->rcm", o_flat.reshape(SEQ_SHARDS, shard_rows, q_cols).astype(jnp.float32), d_out.reshape(SEQ_SHARDS, shard_rows, MODEL_DIM).astype(jnp.float32)).astype(jnp.bfloat16).reshape(SEQ_SHARDS, NUM_HEADS, HEAD_DIM, MODEL_DIM)
    return y_out, grad_x, grad_wq, grad_wk, grad_wv, grad_wo
```

```python
import functools

import jax
import jax.numpy as jnp
from jax import lax
from jax.experimental import pallas as pl
from jax.experimental.pallas import tpu as pltpu
from jax.sharding import PartitionSpec as P

ROW_SPEC = P(("dp", "cp", "tp"), None)
HEAD_SPEC = P(None, "tp", None)
OUT_W_SPEC = P("tp", None, None)
GRAD_SPEC = P(("dp", "cp"), None, "tp", None)
GRAD_OUT_SPEC = P(("dp", "cp"), "tp", None, None)
NT = (((1,), (1,)), ((), ()))
TN = (((0,), (0,)), ((), ()))
NN = (((1,), (0,)), ((), ()))
MESH = pl.DeviceIdType.MESH
VMEM_BYTES = 67_043_328
RS_TILES = 8
CHUNKS = 16
SLOTS = 4


def mm(a, b, dims=NN):
    return lax.dot_general(a, b, dims, preferred_element_type=jnp.float32)


def attention_kernel(tp, cp, *refs):
    (x_ref, dy_ref, wq_ref, wk_ref, wv_ref, wo_ref,
     y_ref, dx_ref, xr_ref, dyr_ref, o_ref, dq_ref, dk_ref, dv_ref,
     wbuf, wf32, wall, wo_all, flat, heads, o_send, g_send, stat, stat_t,
     part, r1, r2, r3, s2,
     w_sem, wo_sem, ag_send, ag_recv, in_send, in_recv, out_send, out_recv,
     r1_send, r1_recv, r2_send, r2_recv, r3_send, r3_recv) = refs
    me_t, me_c = lax.axis_index("tp"), lax.axis_index("cp")
    right, left, across = (me_t + 1) % tp, (me_t + tp - 1) % tp, (me_t + 2) % tp
    rb, dm = x_ref.shape
    rows = rb * tp
    half = rows // 2
    cols = dm // 2
    total, hd = heads.shape[1:]
    n_heads = cp
    scale = hd ** -0.5

    w_refs = (wq_ref, wk_ref, wv_ref)
    chunk = dm // CHUNKS

    def w_copy(t, c, slot):
        return pltpu.make_async_copy(w_refs[t].at[pl.ds(c * chunk * n_heads, chunk * n_heads)], wbuf.at[slot], w_sem.at[slot])

    for c in range(SLOTS):
        w_copy(0, c, c).start()

    barrier = pltpu.get_barrier_semaphore()
    for t_dev in (left, right):
        pl.semaphore_signal(barrier, inc=1, device_id={"tp": t_dev}, device_id_type=MESH)
    for k in range(1, cp):
        pl.semaphore_signal(barrier, inc=1, device_id={"cp": (me_c + k) % cp}, device_id_type=MESH)
    pl.semaphore_wait(barrier, 2 + cp - 1)

    def gather_copy(src, dst, which, idx, block, col_half, to):
        where = (pl.ds(block * rb, rb), pl.ds(col_half * cols, cols))
        src_view = src.at[:, pl.ds(col_half * cols, cols)] if src is not dst else dst.at[where]
        return pltpu.make_async_remote_copy(src_view, dst.at[where], ag_send.at[which, idx], ag_recv.at[which, idx],
                                            device_id={"tp": to}, device_id_type=MESH)

    def gather_start(which, src, dst):
        for idx, col_half, to in ((0, 0, right), (1, 1, left), (2, 1, right), (3, 0, left)):
            gather_copy(src, dst, which, idx, me_t, col_half, to).start()
        dst[pl.ds(pl.multiple_of(me_t * rb, rb), rb), :] = src[...]

    def gather_pass(which, src, dst):
        gather_copy(src, dst, which, 0, left, 0, right).wait_recv()
        gather_copy(dst, dst, which, 4, left, 0, right).start()
        gather_copy(src, dst, which, 1, right, 1, left).wait_recv()
        gather_copy(dst, dst, which, 5, right, 1, left).start()

    def gather_end(which, src, dst):
        gather_copy(src, dst, which, 2, left, 1, right).wait_recv()
        gather_copy(src, dst, which, 3, right, 0, left).wait_recv()
        gather_copy(dst, dst, which, 4, across, 0, right).wait_recv()
        gather_copy(dst, dst, which, 5, across, 1, left).wait_recv()

    def relayout(t):
        @pl.loop(0, CHUNKS)
        def _(c):
            slot = c % SLOTS
            w_copy(t, c, slot).wait()
            wf32[...] = wbuf[slot].astype(jnp.float32)
            at = pl.ds(pl.multiple_of(c * chunk, chunk), chunk)
            for h in range(n_heads):
                wall[t, at, h * hd:(h + 1) * hd] = wf32[pl.ds(h, chunk, stride=n_heads), :].astype(jnp.bfloat16)

            @pl.when(c + SLOTS < CHUNKS)
            def _():
                w_copy(t, c + SLOTS, slot).start()

            if t + 1 < len(w_refs):
                @pl.when(c + SLOTS >= CHUNKS)
                def _():
                    w_copy(t + 1, c + SLOTS - CHUNKS, slot).start()

    gather_start(0, x_ref, xr_ref)
    relayout(0)
    gather_pass(0, x_ref, xr_ref)
    gather_start(1, dy_ref, dyr_ref)
    relayout(1)
    wo_copy = pltpu.make_async_copy(wo_ref, wo_all, wo_sem)
    wo_copy.start()
    relayout(2)
    gather_end(0, x_ref, xr_ref)
    gather_pass(1, dy_ref, dyr_ref)

    def send_in(t, h):
        for part_half in range(2):
            block = me_c if part_half == 0 else 2 * cp - 1 - me_c
            src = flat.at[t, pl.ds(part_half * half, half), pl.ds(pl.multiple_of(h * hd, hd), hd)]
            dst = heads.at[t, pl.ds(pl.multiple_of(block * half, half), half)]

            @pl.when(h == me_c)
            def _():
                pltpu.make_async_copy(src, dst, in_recv.at[t]).start()

            @pl.when(h != me_c)
            def _():
                pltpu.make_async_remote_copy(src, dst, in_send.at[t], in_recv.at[t],
                                             device_id={"cp": h}, device_id_type=MESH).start()

    def wait_in(t):
        pltpu.make_async_copy(heads.at[t], heads.at[t], in_recv.at[t]).wait()

    pairs = cp // 2

    @pl.loop(0, 3 * pairs)
    def _(i):
        t = i // pairs
        pair = (me_c // 2 + 1 + i % pairs) % pairs
        at = pl.ds(pl.multiple_of(pair * 2 * hd, 2 * hd), 2 * hd)
        flat[t, :, at] = mm(xr_ref[...], wall[t, :, at]).astype(jnp.bfloat16)
        for e in range(2):
            send_in(t, pair * 2 + e)

    gather_end(1, dy_ref, dyr_ref)
    wo_copy.wait()

    @pl.loop(0, pairs)
    def _(i):
        pair = (me_c // 2 + 1 + i) % pairs
        at = pl.ds(pl.multiple_of(pair * 2 * hd, 2 * hd), 2 * hd)
        flat[3, :, at] = mm(dyr_ref[...], wo_all[at, :], NT).astype(jnp.bfloat16)
        for e in range(2):
            send_in(3, pair * 2 + e)

    outs = (o_ref, dq_ref, dk_ref, dv_ref)

    def send_out(t, src_ref, start, count):
        for b in range(start // half, (start + count) // half):
            s, part_half = (b, 0) if b < cp else (2 * cp - 1 - b, 1)
            src = src_ref.at[pl.ds(b * half, half)]
            dst = outs[t].at[pl.ds(part_half * half, half), pl.ds(pl.multiple_of(me_c * hd, hd), hd)]

            @pl.when(me_c == s)
            def _():
                pltpu.make_async_copy(src, dst, out_recv.at[t]).start()

            @pl.when(me_c != s)
            def _():
                pltpu.make_async_remote_copy(src, dst, out_send.at[t], out_recv.at[t],
                                             device_id={"cp": s}, device_id_type=MESH).start()

    def wait_out(t):
        pltpu.make_async_copy(outs[t], outs[t], out_recv.at[t]).wait()

    qb = min(256, total)
    blocks = total // qb

    def causal(shape, q_start, k_start, q_axis):
        q_pos = lax.broadcasted_iota(jnp.int32, shape, q_axis) + q_start
        k_pos = lax.broadcasted_iota(jnp.int32, shape, 1 - q_axis) + k_start
        return q_pos >= k_pos

    for t in range(3):
        wait_in(t)
    for i in range(blocks):
        at, n = pl.ds(i * qb, qb), (i + 1) * qb
        s = mm(heads[0, at, :], heads[1, :n, :], NT) * scale
        s = jnp.where(causal(s.shape, i * qb, 0, 0), s, -jnp.inf)
        m = jnp.max(s, axis=1, keepdims=True)
        p = jnp.exp(s - m)
        l = jnp.sum(p, axis=1, keepdims=True)
        o = mm(p.astype(jnp.bfloat16), heads[2, :n, :]) / l
        o_send[at, :] = o.astype(jnp.bfloat16)
        stat[0, at, :] = jnp.broadcast_to(m + jnp.log(l), (qb, hd))
        send_out(0, o_send, i * qb, qb)

    wait_in(3)
    for i in range(blocks):
        at = pl.ds(i * qb, qb)
        delta = jnp.sum(heads[3, at, :].astype(jnp.float32) * o_send[at, :].astype(jnp.float32), axis=1, keepdims=True)
        stat[1, at, :] = jnp.broadcast_to(delta, (qb, hd))
    for j in range(2):
        for i in range(total // hd):
            stat_t[j, :, i * hd:(i + 1) * hd] = stat[j, i * hd:(i + 1) * hd, :].T[:8]

    for i in range(blocks):
        at, n = pl.ds(i * qb, qb), (i + 1) * qb
        s = mm(heads[0, at, :], heads[1, :n, :], NT) * scale
        p = jnp.where(causal(s.shape, i * qb, 0, 0), jnp.exp(s - stat[0, at, :1]), 0.0)
        dp = mm(heads[3, at, :], heads[2, :n, :], NT)
        ds = (p * (dp - stat[1, at, :1])).astype(jnp.bfloat16)
        g_send[0, at, :] = (mm(ds, heads[1, :n, :]) * scale).astype(jnp.bfloat16)
        send_out(1, g_send.at[0], i * qb, qb)
    for i in range(blocks):
        at, after = pl.ds(i * qb, qb), pl.ds(i * qb, total - i * qb)
        s = mm(heads[1, at, :], heads[0, after, :], NT) * scale
        p = jnp.where(causal(s.shape, 0, 0, 1), jnp.exp(s - stat_t[0, :1, after]), 0.0)
        dp = mm(heads[2, at, :], heads[3, after, :], NT)
        ds = (p * (dp - stat_t[1, :1, after])).astype(jnp.bfloat16)
        g_send[2, at, :] = mm(p.astype(jnp.bfloat16), heads[3, after, :]).astype(jnp.bfloat16)
        send_out(3, g_send.at[2], i * qb, qb)
        g_send[1, at, :] = (mm(ds, heads[0, after, :]) * scale).astype(jnp.bfloat16)
        send_out(2, g_send.at[1], i * qb, qb)

    width = dm // RS_TILES

    def rs_parts(j, tile, odd):
        onward, back = (left, right) if odd else (right, left)
        at = pl.ds(pl.multiple_of(tile * width, width), width)

        def mine(d):
            return (j, pl.ds(pl.multiple_of(d * rb, rb), rb), at)

        def copy(src, dst, send, recv, to):
            return pltpu.make_async_remote_copy(src, dst.at[j, tile], send.at[j, tile], recv.at[j, tile],
                                                device_id={"tp": to}, device_id_type=MESH)

        first = lambda: copy(part.at[mine(across)], r1, r1_send, r1_recv, onward)
        second = lambda: copy(s2.at[j, tile], r2, r2_send, r2_recv, onward)
        direct = lambda: copy(part.at[mine(back)], r3, r3_send, r3_recv, back)
        return at, mine, onward, first, second, direct

    def reduce_start(j, compute):
        @pl.loop(0, RS_TILES // 2)
        def _(i):
            for odd in range(2):
                tile = i * 2 + odd
                at, _, _, first, _, _ = rs_parts(j, tile, odd)
                part[j, :, at] = compute(at)
                first().start()

        @pl.loop(0, RS_TILES // 2)
        def _(i):
            for odd in range(2):
                rs_parts(j, i * 2 + odd, odd)[5]().start()

        @pl.loop(0, RS_TILES // 2)
        def _(i):
            for odd in range(2):
                tile = i * 2 + odd
                _, mine, onward, first, second, _ = rs_parts(j, tile, odd)
                first().wait_recv()
                s2[j, tile] = r1[j, tile] + part[mine(onward)]
                second().start()

    def reduce_end(j, out):
        @pl.loop(0, RS_TILES // 2)
        def _(i):
            for odd in range(2):
                tile = i * 2 + odd
                at, mine, _, first, second, direct = rs_parts(j, tile, odd)
                direct().wait_recv()
                second().wait_recv()
                out[:, at] = (part[mine(me_t)] + r2[j, tile] + r3[j, tile]).astype(jnp.bfloat16)
                first().wait_send()
                second().wait_send()
                direct().wait_send()

    wait_out(0)
    reduce_start(0, lambda at: mm(o_ref[...], wo_all[:, at]))
    for t in range(1, 4):
        wait_out(t)
    reduce_start(1, lambda at: mm(dq_ref[...], wall[0, at, :], NT) + mm(dk_ref[...], wall[1, at, :], NT) + mm(dv_ref[...], wall[2, at, :], NT))
    reduce_end(0, y_ref)
    reduce_end(1, dx_ref)

    others = heads.at[0, pl.ds(0, (cp - 1) * rows)]
    for t in range(4):
        for sem in (in_send, out_send):
            pltpu.make_async_copy(others, others, sem.at[t]).wait()
    for which, src, dst in ((0, x_ref, xr_ref), (1, dy_ref, dyr_ref)):
        for idx, col_half, to in ((0, 0, right), (1, 1, left), (2, 1, right), (3, 0, left)):
            gather_copy(src, dst, which, idx, me_t, col_half, to).wait_send()
        gather_copy(dst, dst, which, 4, left, 0, right).wait_send()
        gather_copy(dst, dst, which, 5, right, 1, left).wait_send()


def attention_call(tp, cp, x_blk, dy_blk, wq, wk, wv, wo):
    rb, dm = x_blk.shape
    rows = rb * tp
    hc, _ = wo.shape
    hd = hc // cp
    total = rows * cp
    bf, f32 = jnp.bfloat16, jnp.float32
    chunk = dm // CHUNKS
    width = dm // RS_TILES
    vmem, hbm = pl.BlockSpec(memory_space=pltpu.VMEM), pl.BlockSpec(memory_space=pl.ANY)
    out = lambda r, c: jax.ShapeDtypeStruct((r, c), bf)
    dma = pltpu.SemaphoreType.DMA
    return pl.pallas_call(
        functools.partial(attention_kernel, tp, cp),
        out_shape=(out(rb, dm), out(rb, dm), out(rows, dm), out(rows, dm), out(rows, hc), out(rows, hc), out(rows, hc), out(rows, hc)),
        in_specs=[vmem, vmem, hbm, hbm, hbm, hbm],
        out_specs=[vmem] * 8,
        scratch_shapes=[
            pltpu.VMEM((SLOTS, chunk * cp, hd), bf), pltpu.VMEM((chunk * cp, hd), f32),
            pltpu.VMEM((3, dm, hc), bf), pltpu.VMEM((hc, dm), bf),
            pltpu.VMEM((4, rows, hc), bf), pltpu.VMEM((4, total, hd), bf),
            pltpu.VMEM((total, hd), bf), pltpu.VMEM((3, total, hd), bf),
            pltpu.VMEM((2, total, hd), f32), pltpu.VMEM((2, 8, total), f32),
            pltpu.VMEM((2, rows, dm), f32),
            pltpu.VMEM((2, RS_TILES, rb, width), f32), pltpu.VMEM((2, RS_TILES, rb, width), f32),
            pltpu.VMEM((2, RS_TILES, rb, width), f32), pltpu.VMEM((2, RS_TILES, rb, width), f32),
            dma((SLOTS,)), dma, dma((2, 6)), dma((2, 6)), dma((4,)), dma((4,)), dma((4,)), dma((4,)),
            dma((2, RS_TILES)), dma((2, RS_TILES)), dma((2, RS_TILES)), dma((2, RS_TILES)), dma((2, RS_TILES)), dma((2, RS_TILES)),
        ],
        compiler_params=pltpu.CompilerParams(collective_id=0, has_side_effects=True, vmem_limit_bytes=VMEM_BYTES),
    )(x_blk, dy_blk, wq, wk, wv, wo)


def grad_kernel(n_heads, x_ref, dy_ref, o_ref, dq_ref, dk_ref, dv_ref, gq_ref, gk_ref, gv_ref, go_ref, wide):
    hd = wide.shape[1]
    m_tile = x_ref.shape[1]
    for d_ref, g_ref in ((dq_ref, gq_ref), (dk_ref, gk_ref), (dv_ref, gv_ref)):
        grad = mm(x_ref[...], d_ref[...], TN)
        for h in range(n_heads):
            wide[pl.ds(h, m_tile, stride=n_heads), :] = grad[:, h * hd:(h + 1) * hd]
        g_ref[...] = wide[...].astype(jnp.bfloat16)
    go_ref[...] = mm(o_ref[...], dy_ref[...], TN).astype(jnp.bfloat16)


def grad_call(n_heads, x_rows, dy_rows, o_flat, dq, dk, dv):
    rows, dm = x_rows.shape
    hc = o_flat.shape[1]
    hd = hc // n_heads
    steps = n_heads
    m_tile, o_tile = dm // steps, hc // steps
    bf = jnp.bfloat16
    whole = lambda c: pl.BlockSpec((rows, c), lambda i: (0, 0))
    tiled = pl.BlockSpec((m_tile * n_heads, hd), lambda i: (i, 0))
    return pl.pallas_call(
        functools.partial(grad_kernel, n_heads),
        out_shape=[jax.ShapeDtypeStruct((dm * n_heads, hd), bf)] * 3 + [jax.ShapeDtypeStruct((hc, dm), bf)],
        grid=(steps,),
        in_specs=[pl.BlockSpec((rows, m_tile), lambda i: (0, i)), whole(dm), pl.BlockSpec((rows, o_tile), lambda i: (0, i)),
                  whole(hc), whole(hc), whole(hc)],
        out_specs=[tiled] * 3 + [pl.BlockSpec((o_tile, dm), lambda i: (i, 0))],
        scratch_shapes=[pltpu.VMEM((m_tile * n_heads, hd), jnp.float32)],
        compiler_params=pltpu.CompilerParams(vmem_limit_bytes=VMEM_BYTES),
    )(x_rows, dy_rows, o_flat, dq, dk, dv)


def solution(mesh):
    tp, cp = mesh.shape["tp"], mesh.shape["cp"]

    def device_fn(x_blk, w_query, w_key, w_value, w_out, dy_blk):
        dm, n_heads, hd = w_query.shape
        if tp != 4 or n_heads != cp or w_key.shape != w_query.shape:
            raise ValueError("unsupported split")
        tall = lambda w: w.reshape(dm * n_heads, hd)
        y_blk, dx_blk, x_rows, dy_rows, o_flat, dq, dk, dv = attention_call(
            tp, cp, x_blk, dy_blk, tall(w_query), tall(w_key), tall(w_value), w_out.reshape(n_heads * hd, dm))
        gq, gk, gv, go = grad_call(n_heads, x_rows, dy_rows, o_flat, dq, dk, dv)
        split = lambda g: g.reshape(1, dm, n_heads, hd)
        return y_blk, dx_blk, split(gq), split(gk), split(gv), go.reshape(1, n_heads, hd, dm)

    return jax.shard_map(device_fn, mesh=mesh,
                         in_specs=(ROW_SPEC, HEAD_SPEC, HEAD_SPEC, HEAD_SPEC, OUT_W_SPEC, ROW_SPEC),
                         out_specs=(ROW_SPEC, ROW_SPEC, GRAD_SPEC, GRAD_SPEC, GRAD_SPEC, GRAD_OUT_SPEC),
                         check_vma=False)
```

```python
import functools

import jax
import jax.numpy as jnp
from jax import lax
from jax.experimental import pallas as pl
from jax.experimental.pallas import tpu as pltpu
from jax.sharding import PartitionSpec as P

ROW_SPEC = P(("dp", "cp", "tp"), None)
HEAD_SPEC = P(None, "tp", None)
OUT_W_SPEC = P("tp", None, None)
GRAD_SPEC = P(("dp", "cp"), None, "tp", None)
GRAD_OUT_SPEC = P(("dp", "cp"), "tp", None, None)
NT = (((1,), (1,)), ((), ()))
TN = (((0,), (0,)), ((), ()))
NN = (((1,), (0,)), ((), ()))
MESH = pl.DeviceIdType.MESH
VMEM_BYTES = 67_043_328
RS_TILES = 8
CHUNKS = 16
SLOTS = 4


def mm(a, b, dims=NN):
    return lax.dot_general(a, b, dims, preferred_element_type=jnp.float32)


def attention_kernel(tp, cp, *refs):
    (x_ref, dy_ref, wq_ref, wk_ref, wv_ref, wo_ref,
     y_ref, own_ref, far_r, far_l, back_l, back_r, on_r, on_l, xr_ref, dyr_ref, o_ref, dq_ref, dk_ref, dv_ref,
     wbuf, wf32, wall, wo_all, flat, heads, o_send, g_send, stat, stat_t,
     part, dx_part, r1, r2, r3, s2,
     w_sem, wo_sem, ag_send, ag_recv, in_send, in_recv, out_send, out_recv,
     r1_send, r1_recv, r2_send, r2_recv, r3_send, r3_recv) = refs
    me_t, me_c = lax.axis_index("tp"), lax.axis_index("cp")
    right, left, across = (me_t + 1) % tp, (me_t + tp - 1) % tp, (me_t + 2) % tp
    rb, dm = x_ref.shape
    rows = rb * tp
    half = rows // 2
    cols = dm // 2
    total, hd = heads.shape[1:]
    n_heads = cp
    scale = hd ** -0.5

    w_refs = (wq_ref, wk_ref, wv_ref)
    chunk = dm // CHUNKS

    def w_copy(t, c, slot):
        return pltpu.make_async_copy(w_refs[t].at[pl.ds(c * chunk * n_heads, chunk * n_heads)], wbuf.at[slot], w_sem.at[slot])

    for c in range(SLOTS):
        w_copy(0, c, c).start()

    barrier = pltpu.get_barrier_semaphore()
    for t_dev in (left, right):
        pl.semaphore_signal(barrier, inc=1, device_id={"tp": t_dev}, device_id_type=MESH)
    for k in range(1, cp):
        pl.semaphore_signal(barrier, inc=1, device_id={"cp": (me_c + k) % cp}, device_id_type=MESH)
    pl.semaphore_wait(barrier, 2 + cp - 1)

    def gather_copy(src, dst, which, idx, block, col_half, to):
        where = (pl.ds(block * rb, rb), pl.ds(col_half * cols, cols))
        src_view = src.at[:, pl.ds(col_half * cols, cols)] if src is not dst else dst.at[where]
        return pltpu.make_async_remote_copy(src_view, dst.at[where], ag_send.at[which, idx], ag_recv.at[which, idx],
                                            device_id={"tp": to}, device_id_type=MESH)

    def gather_start(which, src, dst):
        for idx, col_half, to in ((0, 0, right), (1, 1, left), (2, 1, right), (3, 0, left)):
            gather_copy(src, dst, which, idx, me_t, col_half, to).start()
        dst[pl.ds(pl.multiple_of(me_t * rb, rb), rb), :] = src[...]

    def gather_pass(which, src, dst):
        gather_copy(src, dst, which, 0, left, 0, right).wait_recv()
        gather_copy(dst, dst, which, 4, left, 0, right).start()
        gather_copy(src, dst, which, 1, right, 1, left).wait_recv()
        gather_copy(dst, dst, which, 5, right, 1, left).start()

    def gather_end(which, src, dst):
        gather_copy(src, dst, which, 2, left, 1, right).wait_recv()
        gather_copy(src, dst, which, 3, right, 0, left).wait_recv()
        gather_copy(dst, dst, which, 4, across, 0, right).wait_recv()
        gather_copy(dst, dst, which, 5, across, 1, left).wait_recv()

    def relayout(t):
        @pl.loop(0, CHUNKS)
        def _(c):
            slot = c % SLOTS
            w_copy(t, c, slot).wait()
            wf32[...] = wbuf[slot].astype(jnp.float32)
            at = pl.ds(pl.multiple_of(c * chunk, chunk), chunk)
            for h in range(n_heads):
                wall[t, at, h * hd:(h + 1) * hd] = wf32[pl.ds(h, chunk, stride=n_heads), :].astype(jnp.bfloat16)

            @pl.when(c + SLOTS < CHUNKS)
            def _():
                w_copy(t, c + SLOTS, slot).start()

            if t + 1 < len(w_refs):
                @pl.when(c + SLOTS >= CHUNKS)
                def _():
                    w_copy(t + 1, c + SLOTS - CHUNKS, slot).start()

    gather_start(0, x_ref, xr_ref)
    relayout(0)
    gather_pass(0, x_ref, xr_ref)
    gather_start(1, dy_ref, dyr_ref)
    relayout(1)
    wo_copy = pltpu.make_async_copy(wo_ref, wo_all, wo_sem)
    wo_copy.start()
    relayout(2)
    gather_end(0, x_ref, xr_ref)
    gather_pass(1, dy_ref, dyr_ref)

    def send_in(t, h):
        for part_half in range(2):
            block = me_c if part_half == 0 else 2 * cp - 1 - me_c
            src = flat.at[t, pl.ds(part_half * half, half), pl.ds(pl.multiple_of(h * hd, hd), hd)]
            dst = heads.at[t, pl.ds(pl.multiple_of(block * half, half), half)]

            @pl.when(h == me_c)
            def _():
                pltpu.make_async_copy(src, dst, in_recv.at[t]).start()

            @pl.when(h != me_c)
            def _():
                pltpu.make_async_remote_copy(src, dst, in_send.at[t], in_recv.at[t],
                                             device_id={"cp": h}, device_id_type=MESH).start()

    def wait_in(t):
        pltpu.make_async_copy(heads.at[t], heads.at[t], in_recv.at[t]).wait()

    pairs = cp // 2

    @pl.loop(0, 3 * pairs)
    def _(i):
        t = i // pairs
        pair = (me_c // 2 + 1 + i % pairs) % pairs
        at = pl.ds(pl.multiple_of(pair * 2 * hd, 2 * hd), 2 * hd)
        flat[t, :, at] = mm(xr_ref[...], wall[t, :, at]).astype(jnp.bfloat16)
        for e in range(2):
            send_in(t, pair * 2 + e)

    gather_end(1, dy_ref, dyr_ref)
    wo_copy.wait()

    @pl.loop(0, pairs)
    def _(i):
        pair = (me_c // 2 + 1 + i) % pairs
        at = pl.ds(pl.multiple_of(pair * 2 * hd, 2 * hd), 2 * hd)
        flat[3, :, at] = mm(dyr_ref[...], wo_all[at, :], NT).astype(jnp.bfloat16)
        for e in range(2):
            send_in(3, pair * 2 + e)

    outs = (o_ref, dq_ref, dk_ref, dv_ref)

    def send_out(t, src_ref, start, count):
        for b in range(start // half, (start + count) // half):
            s, part_half = (b, 0) if b < cp else (2 * cp - 1 - b, 1)
            src = src_ref.at[pl.ds(b * half, half)]
            dst = outs[t].at[pl.ds(part_half * half, half), pl.ds(pl.multiple_of(me_c * hd, hd), hd)]

            @pl.when(me_c == s)
            def _():
                pltpu.make_async_copy(src, dst, out_recv.at[t]).start()

            @pl.when(me_c != s)
            def _():
                pltpu.make_async_remote_copy(src, dst, out_send.at[t], out_recv.at[t],
                                             device_id={"cp": s}, device_id_type=MESH).start()

    def wait_out(t):
        pltpu.make_async_copy(outs[t], outs[t], out_recv.at[t]).wait()

    qb = min(256, total)
    blocks = total // qb

    def causal(shape, q_start, k_start, q_axis):
        q_pos = lax.broadcasted_iota(jnp.int32, shape, q_axis) + q_start
        k_pos = lax.broadcasted_iota(jnp.int32, shape, 1 - q_axis) + k_start
        return q_pos >= k_pos

    for t in range(3):
        wait_in(t)
    for i in range(blocks):
        at, n = pl.ds(i * qb, qb), (i + 1) * qb
        s = mm(heads[0, at, :], heads[1, :n, :], NT) * scale
        s = jnp.where(causal(s.shape, i * qb, 0, 0), s, -jnp.inf)
        m = jnp.max(s, axis=1, keepdims=True)
        p = jnp.exp(s - m)
        l = jnp.sum(p, axis=1, keepdims=True)
        o = mm(p.astype(jnp.bfloat16), heads[2, :n, :]) / l
        o_send[at, :] = o.astype(jnp.bfloat16)
        stat[0, at, :] = jnp.broadcast_to(m + jnp.log(l), (qb, hd))
        send_out(0, o_send, i * qb, qb)

    wait_in(3)
    for i in range(blocks):
        at = pl.ds(i * qb, qb)
        delta = jnp.sum(heads[3, at, :].astype(jnp.float32) * o_send[at, :].astype(jnp.float32), axis=1, keepdims=True)
        stat[1, at, :] = jnp.broadcast_to(delta, (qb, hd))
    for j in range(2):
        for i in range(total // hd):
            stat_t[j, :, i * hd:(i + 1) * hd] = stat[j, i * hd:(i + 1) * hd, :].T[:8]

    for i in range(blocks):
        at, n = pl.ds(i * qb, qb), (i + 1) * qb
        s = mm(heads[0, at, :], heads[1, :n, :], NT) * scale
        p = jnp.where(causal(s.shape, i * qb, 0, 0), jnp.exp(s - stat[0, at, :1]), 0.0)
        dp = mm(heads[3, at, :], heads[2, :n, :], NT)
        ds = (p * (dp - stat[1, at, :1])).astype(jnp.bfloat16)
        g_send[0, at, :] = (mm(ds, heads[1, :n, :]) * scale).astype(jnp.bfloat16)
        send_out(1, g_send.at[0], i * qb, qb)
    width = dm // RS_TILES

    def rs_parts(tile, odd):
        onward, back = (left, right) if odd else (right, left)
        at = pl.ds(pl.multiple_of(tile * width, width), width)

        def mine(d):
            return (pl.ds(pl.multiple_of(d * rb, rb), rb), at)

        def copy(src, dst, send, recv, to):
            return pltpu.make_async_remote_copy(src, dst.at[tile], send.at[tile], recv.at[tile],
                                                device_id={"tp": to}, device_id_type=MESH)

        first = lambda: copy(part.at[mine(across)], r1, r1_send, r1_recv, onward)
        second = lambda: copy(s2.at[tile], r2, r2_send, r2_recv, onward)
        direct = lambda: copy(part.at[mine(back)], r3, r3_send, r3_recv, back)
        return at, mine, onward, first, second, direct

    def pairs_of_tiles(step):
        @pl.loop(0, RS_TILES // 2)
        def _(i):
            for odd in range(2):
                step(i * 2 + odd, odd)

    def reduce_first(tile, odd):
        at, _, _, first, _, _ = rs_parts(tile, odd)
        part[:, at] = mm(o_ref[...], wo_all[:, at])
        first().start()

    def reduce_direct(tile, odd):
        rs_parts(tile, odd)[5]().start()

    def reduce_second(tile, odd):
        _, mine, onward, first, second, _ = rs_parts(tile, odd)
        first().wait_recv()
        s2[tile] = r1[tile] + part[mine(onward)]
        second().start()

    def reduce_last(tile, odd):
        at, mine, _, first, second, direct = rs_parts(tile, odd)
        direct().wait_recv()
        second().wait_recv()
        y_ref[:, at] = (part[mine(me_t)] + r2[tile] + r3[tile]).astype(jnp.bfloat16)
        first().wait_send()
        second().wait_send()
        direct().wait_send()

    wait_out(0)
    pairs_of_tiles(reduce_first)
    pairs_of_tiles(reduce_direct)
    for i in range(blocks):
        at, after = pl.ds(i * qb, qb), pl.ds(i * qb, total - i * qb)
        s = mm(heads[1, at, :], heads[0, after, :], NT) * scale
        p = jnp.where(causal(s.shape, 0, 0, 1), jnp.exp(s - stat_t[0, :1, after]), 0.0)
        dp = mm(heads[2, at, :], heads[3, after, :], NT)
        ds = (p * (dp - stat_t[1, :1, after])).astype(jnp.bfloat16)
        g_send[2, at, :] = mm(p.astype(jnp.bfloat16), heads[3, after, :]).astype(jnp.bfloat16)
        send_out(3, g_send.at[2], i * qb, qb)
        g_send[1, at, :] = (mm(ds, heads[0, after, :]) * scale).astype(jnp.bfloat16)
        send_out(2, g_send.at[1], i * qb, qb)

    pairs_of_tiles(reduce_second)

    for t in range(1, 4):
        wait_out(t)

    def dx_tile(tile, outs_of):
        at = pl.ds(pl.multiple_of(tile * width, width), width)
        dx_part[...] = (mm(dq_ref[...], wall[0, at, :], NT) + mm(dk_ref[...], wall[1, at, :], NT)
                        + mm(dv_ref[...], wall[2, at, :], NT))
        own_ref[:, at] = dx_part[pl.ds(pl.multiple_of(me_t * rb, rb), rb), :]
        for ref, d in outs_of:
            ref[:, pl.ds(pl.multiple_of(tile % (RS_TILES // 2) * width, width), width)] = dx_part[pl.ds(pl.multiple_of(d * rb, rb), rb), :]

    @pl.loop(0, RS_TILES // 2)
    def _(i):
        dx_tile(i, ((far_r, across), (back_l, left), (on_r, right)))

    @pl.loop(RS_TILES // 2, RS_TILES)
    def _(i):
        dx_tile(i, ((far_l, across), (back_r, right), (on_l, left)))

    pairs_of_tiles(reduce_last)

    others = heads.at[0, pl.ds(0, (cp - 1) * rows)]
    for t in range(4):
        for sem in (in_send, out_send):
            pltpu.make_async_copy(others, others, sem.at[t]).wait()
    for which, src, dst in ((0, x_ref, xr_ref), (1, dy_ref, dyr_ref)):
        for idx, col_half, to in ((0, 0, right), (1, 1, left), (2, 1, right), (3, 0, left)):
            gather_copy(src, dst, which, idx, me_t, col_half, to).wait_send()
        gather_copy(dst, dst, which, 4, left, 0, right).wait_send()
        gather_copy(dst, dst, which, 5, right, 1, left).wait_send()


def attention_call(tp, cp, x_blk, dy_blk, wq, wk, wv, wo):
    rb, dm = x_blk.shape
    rows = rb * tp
    hc, _ = wo.shape
    hd = hc // cp
    total = rows * cp
    bf, f32 = jnp.bfloat16, jnp.float32
    chunk = dm // CHUNKS
    width = dm // RS_TILES
    vmem, hbm = pl.BlockSpec(memory_space=pltpu.VMEM), pl.BlockSpec(memory_space=pl.ANY)
    out = lambda r, c: jax.ShapeDtypeStruct((r, c), bf)
    wide = lambda c: jax.ShapeDtypeStruct((rb, c), f32)
    dma = pltpu.SemaphoreType.DMA
    return pl.pallas_call(
        functools.partial(attention_kernel, tp, cp),
        out_shape=(out(rb, dm), wide(dm), *[wide(dm // 2)] * 6, out(rows, dm), out(rows, dm), out(rows, hc), out(rows, hc), out(rows, hc), out(rows, hc)),
        in_specs=[vmem, vmem, hbm, hbm, hbm, hbm],
        out_specs=[vmem] * 14,
        scratch_shapes=[
            pltpu.VMEM((SLOTS, chunk * cp, hd), bf), pltpu.VMEM((chunk * cp, hd), f32),
            pltpu.VMEM((3, dm, hc), bf), pltpu.VMEM((hc, dm), bf),
            pltpu.VMEM((4, rows, hc), bf), pltpu.VMEM((4, total, hd), bf),
            pltpu.VMEM((total, hd), bf), pltpu.VMEM((3, total, hd), bf),
            pltpu.VMEM((2, total, hd), f32), pltpu.VMEM((2, 8, total), f32),
            pltpu.VMEM((rows, dm), f32), pltpu.VMEM((rows, width), f32),
            pltpu.VMEM((RS_TILES, rb, width), f32), pltpu.VMEM((RS_TILES, rb, width), f32),
            pltpu.VMEM((RS_TILES, rb, width), f32), pltpu.VMEM((RS_TILES, rb, width), f32),
            dma((SLOTS,)), dma, dma((2, 6)), dma((2, 6)), dma((4,)), dma((4,)), dma((4,)), dma((4,)),
            *[dma((RS_TILES,))] * 6,
        ],
        compiler_params=pltpu.CompilerParams(collective_id=0, has_side_effects=True, vmem_limit_bytes=VMEM_BYTES),
    )(x_blk, dy_blk, wq, wk, wv, wo)


def head_major_grads(n_heads, x_ref, d_refs, g_refs, wide):
    hd = wide.shape[1]
    m_tile = x_ref.shape[1]
    for d_ref, g_ref in zip(d_refs, g_refs):
        grad = mm(x_ref[...], d_ref[...], TN)
        for h in range(n_heads):
            wide[pl.ds(h, m_tile, stride=n_heads), :] = grad[:, h * hd:(h + 1) * hd]
        g_ref[...] = wide[...].astype(jnp.bfloat16)


def grad_kernel_qk(n_heads, x_ref, dq_ref, dk_ref, gq_ref, gk_ref, wide):
    head_major_grads(n_heads, x_ref, (dq_ref, dk_ref), (gq_ref, gk_ref), wide)


def grad_kernel_vo(n_heads, x_ref, dv_ref, o_ref, dy_ref, y_ref, gv_ref, go_ref, y_out, wide):
    head_major_grads(n_heads, x_ref, (dv_ref,), (gv_ref,), wide)
    go_ref[...] = mm(o_ref[...], dy_ref[...], TN).astype(jnp.bfloat16)
    y_out[...] = y_ref[...]


def grad_call(body, n_heads, x_rows, wholes, tall_count, o_flat=None, dy_rows=None, y_blk=None):
    rows, dm = x_rows.shape
    hc = wholes[0].shape[1]
    hd = hc // n_heads
    steps = n_heads
    m_tile, o_tile = dm // steps, hc // steps
    bf = jnp.bfloat16
    whole = lambda a: pl.BlockSpec(a.shape, lambda i: (0, 0))
    args = [x_rows, *wholes]
    in_specs = [pl.BlockSpec((rows, m_tile), lambda i: (0, i)), *map(whole, wholes)]
    out_shape = [jax.ShapeDtypeStruct((dm * n_heads, hd), bf)] * tall_count
    out_specs = [pl.BlockSpec((m_tile * n_heads, hd), lambda i: (i, 0))] * tall_count
    if o_flat is not None:
        args += [o_flat, dy_rows, y_blk]
        in_specs += [pl.BlockSpec((rows, o_tile), lambda i: (0, i)), whole(dy_rows), whole(y_blk)]
        out_shape += [jax.ShapeDtypeStruct((hc, dm), bf), jax.ShapeDtypeStruct(y_blk.shape, bf)]
        out_specs += [pl.BlockSpec((o_tile, dm), lambda i: (i, 0)), whole(y_blk)]
    return pl.pallas_call(
        functools.partial(body, n_heads),
        out_shape=out_shape,
        grid=(steps,),
        in_specs=in_specs,
        out_specs=out_specs,
        scratch_shapes=[pltpu.VMEM((m_tile * n_heads, hd), jnp.float32)],
        compiler_params=pltpu.CompilerParams(vmem_limit_bytes=VMEM_BYTES),
        cost_estimate=pl.CostEstimate(flops=4 * rows * dm * hc, bytes_accessed=4 * dm * hc + 8 * rows * dm, transcendentals=0),
    )(*args)


def solution(mesh):
    tp, cp = mesh.shape["tp"], mesh.shape["cp"]

    def device_fn(x_blk, w_query, w_key, w_value, w_out, dy_blk):
        dm, n_heads, hd = w_query.shape
        if tp != 4 or n_heads != cp or w_key.shape != w_query.shape:
            raise ValueError("unsupported split")
        tall = lambda w: w.reshape(dm * n_heads, hd)
        y_blk, own, far_r, far_l, back_l, back_r, on_r, on_l, x_rows, dy_rows, o_flat, dq, dk, dv = attention_call(
            tp, cp, x_blk, dy_blk, tall(w_query), tall(w_key), tall(w_value), w_out.reshape(n_heads * hd, dm))
        to_right = lambda a: lax.ppermute(a, "tp", [(i, (i + 1) % tp) for i in range(tp)])
        to_left = lambda a: lax.ppermute(a, "tp", [(i, (i - 1) % tp) for i in range(tp)])
        came_r, came_l = to_right(far_r), to_left(far_l)
        direct_a, direct_b = to_left(back_l), to_right(back_r)
        gq, gk = grad_call(grad_kernel_qk, n_heads, x_rows, (dq, dk), 2)
        gq, gk, on_r, on_l = lax.optimization_barrier((gq, gk, on_r, on_l))
        sum_r, sum_l = on_r + came_r, on_l + came_l
        sum_r, sum_l, x_rows = lax.optimization_barrier((sum_r, sum_l, x_rows))
        gv, go, y_blk = grad_call(grad_kernel_vo, n_heads, x_rows, (dv,), 1, o_flat, dy_rows, y_blk)
        last_a, last_b = to_right(sum_r), to_left(sum_l)
        half_cols = dm // 2
        dx_blk = jnp.concatenate([own[:, :half_cols] + direct_a + last_a, own[:, half_cols:] + direct_b + last_b], axis=1).astype(jnp.bfloat16)
        split = lambda g: g.reshape(1, dm, n_heads, hd)
        return y_blk, dx_blk, split(gq), split(gk), split(gv), go.reshape(1, n_heads, hd, dm)

    return jax.shard_map(device_fn, mesh=mesh,
                         in_specs=(ROW_SPEC, HEAD_SPEC, HEAD_SPEC, HEAD_SPEC, OUT_W_SPEC, ROW_SPEC),
                         out_specs=(ROW_SPEC, ROW_SPEC, GRAD_SPEC, GRAD_SPEC, GRAD_SPEC, GRAD_OUT_SPEC),
                         check_vma=False)
```

```python
import functools

import jax
import jax.numpy as jnp
from jax import lax
from jax.experimental import pallas as pl
from jax.experimental.pallas import tpu as pltpu
from jax.sharding import PartitionSpec as P

ROW_SPEC = P(("dp", "cp", "tp"), None)
HEAD_SPEC = P(None, "tp", None)
OUT_W_SPEC = P("tp", None, None)
GRAD_SPEC = P(("dp", "cp"), None, "tp", None)
GRAD_OUT_SPEC = P(("dp", "cp"), "tp", None, None)
NT = (((1,), (1,)), ((), ()))
TN = (((0,), (0,)), ((), ()))
NN = (((1,), (0,)), ((), ()))
MESH = pl.DeviceIdType.MESH
VMEM_BYTES = 67_043_328
RS_TILES = 8
CHUNKS = 16
SLOTS = 8
STRIPS = 4


def mm(a, b, dims=NN):
    return lax.dot_general(a, b, dims, preferred_element_type=jnp.float32)


def attention_kernel(tp, cp, *refs):
    (x_ref, dy_ref, wq_ref, wk_ref, wv_ref, wo_ref,
     y_ref, own_ref, back_l, back_r, on_r, on_l, xr_ref, dyr_ref, o_ref, dq_ref, dk_ref, dv_ref,
     wbuf, wf32, wall, wo_all, flat, heads, sorted_heads, sorted_o, out_heads, stat, stat_t,
     part, dx_part, r1, r2, r3, s2, r4,
     w_sem, wo_sem, ag_send, ag_recv, in_send, in_recv, out_send, out_recv,
     r1_send, r1_recv, r2_send, r2_recv, r3_send, r3_recv, r4_send, r4_recv) = refs
    me_t, me_c = lax.axis_index("tp"), lax.axis_index("cp")
    right, left, across = (me_t + 1) % tp, (me_t + tp - 1) % tp, (me_t + 2) % tp
    rb, dm = x_ref.shape
    rows = rb * tp
    half = rows // 2
    cols = dm // 2
    total, hd = heads.shape[1:]
    n_heads = cp
    scale = hd ** -0.5

    w_refs = (wq_ref, wk_ref, wv_ref)
    others = heads.at[0, pl.ds(0, (cp - 1) * rows)]
    chunk = dm // CHUNKS

    def w_copy(t, c, slot):
        return pltpu.make_async_copy(w_refs[t].at[pl.ds(c * chunk * n_heads, chunk * n_heads)], wbuf.at[slot], w_sem.at[slot])

    for c in range(SLOTS):
        w_copy(0, c, c).start()

    barrier = pltpu.get_barrier_semaphore()
    for t_dev in (left, right):
        pl.semaphore_signal(barrier, inc=1, device_id={"tp": t_dev}, device_id_type=MESH)
    for k in range(1, cp):
        pl.semaphore_signal(barrier, inc=1, device_id={"cp": (me_c + k) % cp}, device_id_type=MESH)
    pl.semaphore_wait(barrier, 2 + cp - 1)

    def gather_copy(src, dst, which, idx, block, col_half, to):
        where = (pl.ds(block * rb, rb), pl.ds(col_half * cols, cols))
        src_view = src.at[:, pl.ds(col_half * cols, cols)] if src is not dst else dst.at[where]
        return pltpu.make_async_remote_copy(src_view, dst.at[where], ag_send.at[which, idx], ag_recv.at[which, idx],
                                            device_id={"tp": to}, device_id_type=MESH)

    def gather_start(which, src, dst):
        for idx, col_half, to in ((0, 0, right), (1, 1, left), (2, 1, right), (3, 0, left)):
            gather_copy(src, dst, which, idx, me_t, col_half, to).start()
        dst[pl.ds(pl.multiple_of(me_t * rb, rb), rb), :] = src[...]

    def gather_pass(which, src, dst):
        gather_copy(src, dst, which, 0, left, 0, right).wait_recv()
        gather_copy(dst, dst, which, 4, left, 0, right).start()
        gather_copy(src, dst, which, 1, right, 1, left).wait_recv()
        gather_copy(dst, dst, which, 5, right, 1, left).start()

    def gather_end(which, src, dst):
        gather_copy(src, dst, which, 2, left, 1, right).wait_recv()
        gather_copy(src, dst, which, 3, right, 0, left).wait_recv()
        gather_copy(dst, dst, which, 4, across, 0, right).wait_recv()
        gather_copy(dst, dst, which, 5, across, 1, left).wait_recv()

    def relayout(t):
        @pl.loop(0, CHUNKS)
        def _(c):
            slot = c % SLOTS
            w_copy(t, c, slot).wait()
            strip = chunk // STRIPS
            for k in range(STRIPS + 1):
                if k < STRIPS:
                    wf32[k] = wbuf[slot, k * strip * n_heads:(k + 1) * strip * n_heads].astype(jnp.float32)
                if k > 0:
                    at = pl.ds(pl.multiple_of(c * chunk + (k - 1) * strip, strip), strip)
                    for h in range(n_heads):
                        wall[t, at, h * hd:(h + 1) * hd] = wf32[k - 1, pl.ds(h, strip, stride=n_heads), :].astype(jnp.bfloat16)

            @pl.when(c + SLOTS < CHUNKS)
            def _():
                w_copy(t, c + SLOTS, slot).start()

            if t + 1 < len(w_refs):
                @pl.when(c + SLOTS >= CHUNKS)
                def _():
                    w_copy(t + 1, c + SLOTS - CHUNKS, slot).start()

    gather_start(0, x_ref, xr_ref)
    relayout(0)
    gather_pass(0, x_ref, xr_ref)
    gather_start(1, dy_ref, dyr_ref)
    relayout(1)
    wo_copy = pltpu.make_async_copy(wo_ref, wo_all, wo_sem)
    wo_copy.start()
    relayout(2)
    gather_end(0, x_ref, xr_ref)
    gather_pass(1, dy_ref, dyr_ref)

    mine_at = pl.ds(pl.multiple_of(me_c * hd, hd), hd)
    my_rows = pl.ds(pl.multiple_of(me_c * rows, rows), rows)

    def send_in(t, h):
        @pl.when(h != me_c)
        def _():
            pltpu.make_async_remote_copy(flat.at[t, :, pl.ds(pl.multiple_of(h * hd, hd), hd)], heads.at[t, my_rows],
                                         in_send.at[t], in_recv.at[t], device_id={"cp": h}, device_id_type=MESH).start()

    order = [s if s < cp else 2 * cp - 1 - s for s in range(2 * cp)]

    def wait_in(t):
        pltpu.make_async_copy(others, others, in_recv.at[t]).wait()
        heads[t, my_rows, :] = flat[t, :, mine_at]
        for b, s in enumerate(order):
            start = s * rows + (half if b >= cp else 0)
            sorted_heads[t, b * half:(b + 1) * half, :] = heads[t, start:start + half, :]

    pairs = cp // 2

    @pl.loop(0, 3 * pairs)
    def _(i):
        t = i // pairs
        pair = (me_c // 2 + 1 + i % pairs) % pairs
        at = pl.ds(pl.multiple_of(pair * 2 * hd, 2 * hd), 2 * hd)
        flat[t, :, at] = mm(xr_ref[...], wall[t, :, at]).astype(jnp.bfloat16)
        for e in range(2):
            send_in(t, pair * 2 + e)

    gather_end(1, dy_ref, dyr_ref)
    wo_copy.wait()

    @pl.loop(0, pairs)
    def _(i):
        pair = (me_c // 2 + 1 + i) % pairs
        at = pl.ds(pl.multiple_of(pair * 2 * hd, 2 * hd), 2 * hd)
        flat[3, :, at] = mm(dyr_ref[...], wo_all[at, :], NT).astype(jnp.bfloat16)
        for e in range(2):
            send_in(3, pair * 2 + e)

    outs = (o_ref, dq_ref, dk_ref, dv_ref)

    def put(t, i, value):
        for k in range(qb // half):
            b = i * (qb // half) + k
            start = order[b] * rows + (half if b >= cp else 0)
            out_heads[t, start:start + half, :] = value[k * half:(k + 1) * half]

    def send_out(t, i):
        done = walk[:walk.index(i) + 1]
        blocks_of = lambda i: range(i * (qb // half), (i + 1) * (qb // half))
        ready = [b for j in done for b in blocks_of(j)]
        now = [order[b] for b in blocks_of(i)]
        for s in sorted({s for s in now if all(b in ready for b in (s, 2 * cp - 1 - s))}):
            @pl.when(me_c != s)
            def _():
                pltpu.make_async_remote_copy(out_heads.at[t, pl.ds(s * rows, rows)], outs[t].at[:, mine_at],
                                             out_send.at[t], out_recv.at[t], device_id={"cp": s}, device_id_type=MESH).start()

    def wait_out(t):
        outs[t][:, mine_at] = out_heads[t, my_rows, :]
        pltpu.make_async_copy(others, others, out_recv.at[t]).wait()

    qb = min(256, total)
    blocks = total // qb
    walk = sorted(range(blocks), key=lambda i: -min(i, blocks - 1 - i))

    def causal(shape, q_start, k_start, q_axis):
        q_pos = lax.broadcasted_iota(jnp.int32, shape, q_axis) + q_start
        k_pos = lax.broadcasted_iota(jnp.int32, shape, 1 - q_axis) + k_start
        return q_pos >= k_pos

    for t in range(3):
        wait_in(t)
    for i in walk:
        at, n = pl.ds(i * qb, qb), (i + 1) * qb
        s = mm(sorted_heads[0, at, :], sorted_heads[1, :n, :], NT) * scale
        s = jnp.where(causal(s.shape, i * qb, 0, 0), s, -jnp.inf)
        m = jnp.max(s, axis=1, keepdims=True)
        p = jnp.exp(s - m)
        l = jnp.sum(p, axis=1, keepdims=True)
        o = mm(p.astype(jnp.bfloat16), sorted_heads[2, :n, :]) / l
        o = o.astype(jnp.bfloat16)
        sorted_o[at, :] = o
        put(0, i, o)
        stat[0, at, :] = jnp.broadcast_to(m + jnp.log(l), (qb, hd))
        send_out(0, i)

    wait_in(3)
    for i in range(blocks):
        at = pl.ds(i * qb, qb)
        delta = jnp.sum(sorted_heads[3, at, :].astype(jnp.float32) * sorted_o[at, :].astype(jnp.float32), axis=1, keepdims=True)
        stat[1, at, :] = jnp.broadcast_to(delta, (qb, hd))
    for j in range(2):
        for i in range(total // hd):
            stat_t[j, :, i * hd:(i + 1) * hd] = stat[j, i * hd:(i + 1) * hd, :].T[:8]

    for i in walk:
        at, n = pl.ds(i * qb, qb), (i + 1) * qb
        s = mm(sorted_heads[0, at, :], sorted_heads[1, :n, :], NT) * scale
        p = jnp.where(causal(s.shape, i * qb, 0, 0), jnp.exp(s - stat[0, at, :1]), 0.0)
        dp = mm(sorted_heads[3, at, :], sorted_heads[2, :n, :], NT)
        ds = (p * (dp - stat[1, at, :1])).astype(jnp.bfloat16)
        put(1, i, (mm(ds, sorted_heads[1, :n, :]) * scale).astype(jnp.bfloat16))
        send_out(1, i)
    width = dm // RS_TILES

    def rs_parts(tile, odd):
        onward, back = (left, right) if odd else (right, left)
        at = pl.ds(pl.multiple_of(tile * width, width), width)

        def mine(d):
            return (pl.ds(pl.multiple_of(d * rb, rb), rb), at)

        def copy(src, dst, send, recv, to):
            return pltpu.make_async_remote_copy(src, dst.at[tile], send.at[tile], recv.at[tile],
                                                device_id={"tp": to}, device_id_type=MESH)

        first = lambda: copy(part.at[mine(across)], r1, r1_send, r1_recv, onward)
        second = lambda: copy(s2.at[tile], r2, r2_send, r2_recv, onward)
        direct = lambda: copy(part.at[mine(back)], r3, r3_send, r3_recv, back)
        return at, mine, onward, first, second, direct

    def pairs_of_tiles(step):
        @pl.loop(0, RS_TILES // 2)
        def _(i):
            for odd in range(2):
                step(i * 2 + odd, odd)

    def reduce_first(tile, odd):
        at, _, _, first, _, _ = rs_parts(tile, odd)
        part[:, at] = mm(o_ref[...], wo_all[:, at])
        first().start()

    def reduce_direct(tile, odd):
        rs_parts(tile, odd)[5]().start()

    def reduce_second(tile, odd):
        _, mine, onward, first, second, _ = rs_parts(tile, odd)
        first().wait_recv()
        s2[tile] = r1[tile] + part[mine(onward)]
        second().start()

    def reduce_last(tile, odd):
        at, mine, _, first, second, direct = rs_parts(tile, odd)
        direct().wait_recv()
        second().wait_recv()
        y_ref[:, at] = (part[mine(me_t)] + r2[tile] + r3[tile]).astype(jnp.bfloat16)
        first().wait_send()
        second().wait_send()
        direct().wait_send()

    wait_out(0)
    pairs_of_tiles(reduce_first)
    pairs_of_tiles(reduce_direct)
    for i in walk:
        at, after = pl.ds(i * qb, qb), pl.ds(i * qb, total - i * qb)
        s = mm(sorted_heads[1, at, :], sorted_heads[0, after, :], NT) * scale
        p = jnp.where(causal(s.shape, 0, 0, 1), jnp.exp(s - stat_t[0, :1, after]), 0.0)
        dp = mm(sorted_heads[2, at, :], sorted_heads[3, after, :], NT)
        ds = (p * (dp - stat_t[1, :1, after])).astype(jnp.bfloat16)
        put(3, i, mm(p.astype(jnp.bfloat16), sorted_heads[3, after, :]).astype(jnp.bfloat16))
        send_out(3, i)
        put(2, i, (mm(ds, sorted_heads[0, after, :]) * scale).astype(jnp.bfloat16))
        send_out(2, i)

    pairs_of_tiles(reduce_second)

    for t in range(1, 4):
        wait_out(t)

    def dx_copy(tile, odd):
        spot = (pl.ds(pl.multiple_of(across * rb, rb), rb), pl.ds(pl.multiple_of((tile + odd * RS_TILES // 2) * width, width), width))
        return pltpu.make_async_remote_copy(dx_part.at[spot], r4.at[odd, tile], r4_send.at[odd, tile], r4_recv.at[odd, tile],
                                            device_id={"tp": left if odd else right}, device_id_type=MESH)

    def block_of(d, at):
        return dx_part[pl.ds(pl.multiple_of(d * rb, rb), rb), at]

    @pl.loop(0, RS_TILES // 2)
    def _(i):
        for odd, (back_ref, back) in enumerate(((back_l, left), (back_r, right))):
            at = pl.ds(pl.multiple_of((i + odd * RS_TILES // 2) * width, width), width)
            dx_part[:, at] = (mm(dq_ref[...], wall[0, at, :], NT) + mm(dk_ref[...], wall[1, at, :], NT)
                              + mm(dv_ref[...], wall[2, at, :], NT))
            dx_copy(i, odd).start()
            own_ref[:, at] = block_of(me_t, at)
            back_ref[:, pl.ds(pl.multiple_of(i * width, width), width)] = block_of(back, at)

    pairs_of_tiles(reduce_last)

    @pl.loop(0, RS_TILES // 2)
    def _(i):
        for odd, (on_ref, onward) in enumerate(((on_r, right), (on_l, left))):
            at = pl.ds(pl.multiple_of((i + odd * RS_TILES // 2) * width, width), width)
            dx_copy(i, odd).wait_recv()
            on_ref[:, pl.ds(pl.multiple_of(i * width, width), width)] = r4[odd, i] + block_of(onward, at)
            dx_copy(i, odd).wait_send()

    for t in range(4):
        for sem in (in_send, out_send):
            pltpu.make_async_copy(others, others, sem.at[t]).wait()
    for which, src, dst in ((0, x_ref, xr_ref), (1, dy_ref, dyr_ref)):
        for idx, col_half, to in ((0, 0, right), (1, 1, left), (2, 1, right), (3, 0, left)):
            gather_copy(src, dst, which, idx, me_t, col_half, to).wait_send()
        gather_copy(dst, dst, which, 4, left, 0, right).wait_send()
        gather_copy(dst, dst, which, 5, right, 1, left).wait_send()


def attention_call(tp, cp, x_blk, dy_blk, wq, wk, wv, wo):
    rb, dm = x_blk.shape
    rows = rb * tp
    hc, _ = wo.shape
    hd = hc // cp
    total = rows * cp
    bf, f32 = jnp.bfloat16, jnp.float32
    chunk = dm // CHUNKS
    width = dm // RS_TILES
    vmem, hbm = pl.BlockSpec(memory_space=pltpu.VMEM), pl.BlockSpec(memory_space=pl.ANY)
    out = lambda r, c: jax.ShapeDtypeStruct((r, c), bf)
    wide = lambda c: jax.ShapeDtypeStruct((rb, c), f32)
    dma = pltpu.SemaphoreType.DMA
    return pl.pallas_call(
        functools.partial(attention_kernel, tp, cp),
        out_shape=(out(rb, dm), wide(dm), *[wide(dm // 2)] * 4, out(rows, dm), out(rows, dm), out(rows, hc), out(rows, hc), out(rows, hc), out(rows, hc)),
        in_specs=[vmem, vmem, hbm, hbm, hbm, hbm],
        out_specs=[vmem] * 12,
        scratch_shapes=[
            pltpu.VMEM((SLOTS, chunk * cp, hd), bf), pltpu.VMEM((STRIPS, chunk // STRIPS * cp, hd), f32),
            pltpu.VMEM((3, dm, hc), bf), pltpu.VMEM((hc, dm), bf),
            pltpu.VMEM((4, rows, hc), bf), pltpu.VMEM((4, total, hd), bf),
            pltpu.VMEM((4, total, hd), bf), pltpu.VMEM((total, hd), bf), pltpu.VMEM((4, total, hd), bf),
            pltpu.VMEM((2, total, hd), f32), pltpu.VMEM((2, 8, total), f32),
            pltpu.VMEM((rows, dm), f32), pltpu.VMEM((rows, dm), f32),
            pltpu.VMEM((RS_TILES, rb, width), f32), pltpu.VMEM((RS_TILES, rb, width), f32),
            pltpu.VMEM((RS_TILES, rb, width), f32), pltpu.VMEM((RS_TILES, rb, width), f32),
            pltpu.VMEM((2, RS_TILES // 2, rb, width), f32),
            dma((SLOTS,)), dma, dma((2, 6)), dma((2, 6)), dma((4,)), dma((4,)), dma((4,)), dma((4,)),
            *[dma((RS_TILES,))] * 6, *[dma((2, RS_TILES // 2))] * 2,
        ],
        compiler_params=pltpu.CompilerParams(collective_id=0, has_side_effects=True, vmem_limit_bytes=VMEM_BYTES),
    )(x_blk, dy_blk, wq, wk, wv, wo)


def grad_kernel(n_heads, x_hbm, dy_hbm, o_hbm, dq_hbm, dk_hbm, dv_hbm, y_ref, gq_ref, gk_ref, gv_ref, go_ref, y_out,
                x_ref, dy_ref, o_ref, dq_ref, dk_ref, dv_ref, wide, grads, out_grad, in_sem, out_sem):
    rows, dm = x_ref.shape
    hd = wide.shape[-1]
    tiles = grads.shape[1]
    m_tile, o_tile = dm // tiles, n_heads * hd // tiles
    loads = [pltpu.make_async_copy(src, dst, in_sem.at[i]) for i, (src, dst) in enumerate(
        ((dq_hbm, dq_ref), (x_hbm, x_ref), (dk_hbm, dk_ref), (dv_hbm, dv_ref), (o_hbm, o_ref), (dy_hbm, dy_ref)))]
    for load in loads:
        load.start()
    y_out[...] = y_ref[...]
    for load in loads[:4]:
        load.wait()

    @pl.loop(0, tiles)
    def _(i):
        at = pl.ds(pl.multiple_of(i * m_tile, m_tile), m_tile)
        tall = pl.ds(pl.multiple_of(i * m_tile * n_heads, m_tile * n_heads), m_tile * n_heads)
        x_t = x_ref[:, at].T
        for t, (d_ref, g_ref) in enumerate(((dq_ref, gq_ref), (dk_ref, gk_ref), (dv_ref, gv_ref))):
            for h in range(0, n_heads, 2):
                grad = mm(x_t, d_ref[:, h * hd:(h + 2) * hd])
                for e in range(2):
                    wide[t, pl.ds(h + e, m_tile, stride=n_heads), :] = grad[:, e * hd:(e + 1) * hd]
            grads[t, i] = wide[t].astype(jnp.bfloat16)
            pltpu.make_async_copy(grads.at[t, i], g_ref.at[tall], out_sem.at[t]).start()

    for load in loads[4:]:
        load.wait()

    @pl.loop(0, tiles)
    def _(i):
        at = pl.ds(pl.multiple_of(i * o_tile, o_tile), o_tile)
        out_grad[at, :] = mm(o_ref[:, at], dy_ref[...], TN).astype(jnp.bfloat16)
        pltpu.make_async_copy(out_grad.at[at], go_ref.at[at], out_sem.at[3]).start()

    for t, g_ref in enumerate((gq_ref, gk_ref, gv_ref, go_ref)):
        pltpu.make_async_copy(g_ref, g_ref, out_sem.at[t]).wait()


def grad_call(n_heads, x_rows, dy_rows, o_flat, dq, dk, dv, y_blk):
    rows, dm = x_rows.shape
    hc = o_flat.shape[1]
    hd = hc // n_heads
    tiles = n_heads
    bf, f32 = jnp.bfloat16, jnp.float32
    hbm, vmem = pl.BlockSpec(memory_space=pl.ANY), pl.BlockSpec(memory_space=pltpu.VMEM)
    inputs = (x_rows, dy_rows, o_flat, dq, dk, dv)
    return pl.pallas_call(
        functools.partial(grad_kernel, n_heads),
        out_shape=[jax.ShapeDtypeStruct((dm * n_heads, hd), bf)] * 3 + [jax.ShapeDtypeStruct((hc, dm), bf), jax.ShapeDtypeStruct(y_blk.shape, bf)],
        in_specs=[hbm] * 6 + [vmem],
        out_specs=[hbm] * 4 + [vmem],
        scratch_shapes=[*[pltpu.VMEM(a.shape, bf) for a in inputs],
                        pltpu.VMEM((3, dm // tiles * n_heads, hd), f32), pltpu.VMEM((3, tiles, dm // tiles * n_heads, hd), bf),
                        pltpu.VMEM((hc, dm), bf), pltpu.SemaphoreType.DMA((6,)), pltpu.SemaphoreType.DMA((4,))],
        compiler_params=pltpu.CompilerParams(vmem_limit_bytes=VMEM_BYTES),
        cost_estimate=pl.CostEstimate(flops=8 * rows * dm * hc, bytes_accessed=8 * dm * hc + 8 * rows * dm, transcendentals=0),
    )(*inputs, y_blk)


def add_kernel(own, direct_a, last_a, direct_b, last_b, dx_ref):
    cols = direct_a.shape[1]
    dx_ref[:, :cols] = (own[:, :cols] + direct_a[...] + last_a[...]).astype(jnp.bfloat16)
    dx_ref[:, cols:] = (own[:, cols:] + direct_b[...] + last_b[...]).astype(jnp.bfloat16)


def solution(mesh):
    tp, cp = mesh.shape["tp"], mesh.shape["cp"]

    def device_fn(x_blk, w_query, w_key, w_value, w_out, dy_blk):
        dm, n_heads, hd = w_query.shape
        if tp != 4 or n_heads != cp or w_key.shape != w_query.shape:
            raise ValueError("unsupported split")
        tall = lambda w: w.reshape(dm * n_heads, hd)
        y_blk, own, back_l, back_r, on_r, on_l, x_rows, dy_rows, o_flat, dq, dk, dv = attention_call(
            tp, cp, x_blk, dy_blk, tall(w_query), tall(w_key), tall(w_value), w_out.reshape(n_heads * hd, dm))
        to_right = lambda a: lax.ppermute(a, "tp", [(i, (i + 1) % tp) for i in range(tp)])
        to_left = lambda a: lax.ppermute(a, "tp", [(i, (i - 1) % tp) for i in range(tp)])
        last_a, last_b, direct_a, direct_b = to_right(on_r), to_left(on_l), to_left(back_l), to_right(back_r)
        gq, gk, gv, go, y_blk = grad_call(n_heads, x_rows, dy_rows, o_flat, dq, dk, dv, y_blk)
        vmem = pl.BlockSpec(memory_space=pltpu.VMEM)
        dx_blk = pl.pallas_call(add_kernel, out_shape=jax.ShapeDtypeStruct(own.shape, jnp.bfloat16), in_specs=[vmem] * 5, out_specs=vmem)(
            own, direct_a, last_a, direct_b, last_b)
        split = lambda g: g.reshape(1, dm, n_heads, hd)
        return y_blk, dx_blk, split(gq), split(gk), split(gv), go.reshape(1, n_heads, hd, dm)

    return jax.shard_map(device_fn, mesh=mesh,
                         in_specs=(ROW_SPEC, HEAD_SPEC, HEAD_SPEC, HEAD_SPEC, OUT_W_SPEC, ROW_SPEC),
                         out_specs=(ROW_SPEC, ROW_SPEC, GRAD_SPEC, GRAD_SPEC, GRAD_SPEC, GRAD_OUT_SPEC),
                         check_vma=False)
```

```python
import functools

import jax
import jax.numpy as jnp
from jax import lax
from jax.experimental import pallas as pl
from jax.experimental.pallas import tpu as pltpu
from jax.sharding import PartitionSpec as P

ROW_SPEC = P(("dp", "cp", "tp"), None)
HEAD_SPEC = P(None, "tp", None)
OUT_W_SPEC = P("tp", None, None)
GRAD_SPEC = P(("dp", "cp"), None, "tp", None)
GRAD_OUT_SPEC = P(("dp", "cp"), "tp", None, None)
NT = (((1,), (1,)), ((), ()))
TN = (((0,), (0,)), ((), ()))
NN = (((1,), (0,)), ((), ()))
MESH = pl.DeviceIdType.MESH
VMEM_BYTES = 67_043_328
RS_TILES = 8
CHUNKS = 16
SLOTS = 8
STRIPS = 4
PITCH = 12


def mm(a, b, dims=NN):
    return lax.dot_general(a, b, dims, preferred_element_type=jnp.float32)


def attention_kernel(tp, cp, *refs):
    (x_ref, dy_ref, wq_ref, wk_ref, wv_ref, wo_ref,
     y_ref, own_ref, back_l, back_r, on_r, on_l, x_out, dy_out, o_ref, dq_ref, dk_ref, dv_ref,
     xr_ref, dyr_ref, wbuf, wf32, wall, wo_all, flat, heads, sorted_heads, sorted_o, out_heads, stat, stat_t,
     part, dx_part, r1, r2, r3, s2, r4,
     w_sem, wo_sem, row_sem, ag_send, ag_recv, in_send, in_recv, out_send, out_recv,
     r1_send, r1_recv, r2_send, r2_recv, r3_send, r3_recv, r4_send, r4_recv) = refs
    me_t, me_c = lax.axis_index("tp"), lax.axis_index("cp")
    right, left, across = (me_t + 1) % tp, (me_t + tp - 1) % tp, (me_t + 2) % tp
    rb, dm = x_ref.shape
    rows = rb * tp
    half = rows // 2
    cols = dm // 2
    total, hd = heads.shape[1:]
    n_heads = cp
    scale = hd ** -0.5

    w_refs = (wq_ref, wk_ref, wv_ref)
    others = heads.at[0, pl.ds(0, (cp - 1) * rows)]
    chunk = dm // CHUNKS

    def w_copy(t, c, slot):
        return pltpu.make_async_copy(w_refs[t].at[pl.ds(c * chunk * n_heads, chunk * n_heads)], wbuf.at[slot], w_sem.at[slot])

    for c in range(SLOTS):
        w_copy(0, c, c).start()

    barrier = pltpu.get_barrier_semaphore()
    for t_dev in (left, right):
        pl.semaphore_signal(barrier, inc=1, device_id={"tp": t_dev}, device_id_type=MESH)
    for k in range(1, cp):
        pl.semaphore_signal(barrier, inc=1, device_id={"cp": (me_c + k) % cp}, device_id_type=MESH)
    pl.semaphore_wait(barrier, 2 + cp - 1)

    def gather_copy(src, dst, which, idx, block, col_half, to):
        where = (pl.ds(block * rb, rb), pl.ds(col_half * cols, cols))
        src_view = src.at[:, pl.ds(col_half * cols, cols)] if src is not dst else dst.at[where]
        return pltpu.make_async_remote_copy(src_view, dst.at[where], ag_send.at[which, idx], ag_recv.at[which, idx],
                                            device_id={"tp": to}, device_id_type=MESH)

    def gather_start(which, src, dst):
        for idx, col_half, to in ((0, 0, right), (1, 1, left), (2, 1, right), (3, 0, left)):
            gather_copy(src, dst, which, idx, me_t, col_half, to).start()
        dst[pl.ds(pl.multiple_of(me_t * rb, rb), rb), :] = src[...]

    def gather_pass(which, src, dst):
        gather_copy(src, dst, which, 0, left, 0, right).wait_recv()
        gather_copy(dst, dst, which, 4, left, 0, right).start()
        gather_copy(src, dst, which, 1, right, 1, left).wait_recv()
        gather_copy(dst, dst, which, 5, right, 1, left).start()

    def gather_end(which, src, dst):
        gather_copy(src, dst, which, 2, left, 1, right).wait_recv()
        gather_copy(src, dst, which, 3, right, 0, left).wait_recv()
        gather_copy(dst, dst, which, 4, across, 0, right).wait_recv()
        gather_copy(dst, dst, which, 5, across, 1, left).wait_recv()

    pitch = wf32.shape[1] // (chunk // STRIPS)

    def relayout(t):
        @pl.loop(0, CHUNKS)
        def _(c):
            slot = c % SLOTS
            w_copy(t, c, slot).wait()
            strip = chunk // STRIPS
            for k in range(STRIPS + 1):
                if k < STRIPS:
                    for r in range(0, strip, 2):
                        at = (k * strip + r) * n_heads
                        pair = wbuf[slot, at:at + 2 * n_heads].astype(jnp.float32)
                        for e in range(2):
                            wf32[k, (r + e) * pitch:(r + e) * pitch + n_heads] = pair[e * n_heads:(e + 1) * n_heads]
                if k > 0:
                    at = pl.ds(pl.multiple_of(c * chunk + (k - 1) * strip, strip), strip)
                    for h in range(n_heads):
                        wall[t, at, h * hd:(h + 1) * hd] = wf32[k - 1, pl.ds(h, strip, stride=pitch), :].astype(jnp.bfloat16)

            @pl.when(c + SLOTS < CHUNKS)
            def _():
                w_copy(t, c + SLOTS, slot).start()

            if t + 1 < len(w_refs):
                @pl.when(c + SLOTS >= CHUNKS)
                def _():
                    w_copy(t + 1, c + SLOTS - CHUNKS, slot).start()

    gather_start(0, x_ref, xr_ref)
    relayout(0)
    gather_pass(0, x_ref, xr_ref)
    gather_start(1, dy_ref, dyr_ref)
    relayout(1)
    wo_copy = pltpu.make_async_copy(wo_ref, wo_all, wo_sem)
    wo_copy.start()
    relayout(2)
    gather_end(0, x_ref, xr_ref)
    x_copy = pltpu.make_async_copy(xr_ref, x_out, row_sem.at[0])
    x_copy.start()
    gather_pass(1, dy_ref, dyr_ref)

    mine_at = pl.ds(pl.multiple_of(me_c * hd, hd), hd)
    my_rows = pl.ds(pl.multiple_of(me_c * rows, rows), rows)

    def send_in(t, h):
        @pl.when(h != me_c)
        def _():
            pltpu.make_async_remote_copy(flat.at[t, :, pl.ds(pl.multiple_of(h * hd, hd), hd)], heads.at[t, my_rows],
                                         in_send.at[t], in_recv.at[t], device_id={"cp": h}, device_id_type=MESH).start()

    order = [s if s < cp else 2 * cp - 1 - s for s in range(2 * cp)]

    def wait_in(t):
        pltpu.make_async_copy(others, others, in_recv.at[t]).wait()
        heads[t, my_rows, :] = flat[t, :, mine_at]
        for b, s in enumerate(order):
            start = s * rows + (half if b >= cp else 0)
            sorted_heads[t, b * half:(b + 1) * half, :] = heads[t, start:start + half, :]

    pairs = cp // 2

    @pl.loop(0, 3 * pairs)
    def _(i):
        t = i // pairs
        pair = (me_c // 2 + 1 + i % pairs) % pairs
        at = pl.ds(pl.multiple_of(pair * 2 * hd, 2 * hd), 2 * hd)
        flat[t, :, at] = mm(xr_ref[...], wall[t, :, at]).astype(jnp.bfloat16)
        for e in range(2):
            send_in(t, pair * 2 + e)

    gather_end(1, dy_ref, dyr_ref)
    dy_copy = pltpu.make_async_copy(dyr_ref, dy_out, row_sem.at[1])
    dy_copy.start()
    wo_copy.wait()

    @pl.loop(0, pairs)
    def _(i):
        pair = (me_c // 2 + 1 + i) % pairs
        at = pl.ds(pl.multiple_of(pair * 2 * hd, 2 * hd), 2 * hd)
        flat[3, :, at] = mm(dyr_ref[...], wo_all[at, :], NT).astype(jnp.bfloat16)
        for e in range(2):
            send_in(3, pair * 2 + e)

    outs = (o_ref, dq_ref, dk_ref, dv_ref)

    def put(t, i, value):
        for k in range(qb // half):
            b = i * (qb // half) + k
            start = order[b] * rows + (half if b >= cp else 0)
            out_heads[t, start:start + half, :] = value[k * half:(k + 1) * half]

    def send_out(t, i):
        done = walk[:walk.index(i) + 1]
        blocks_of = lambda i: range(i * (qb // half), (i + 1) * (qb // half))
        ready = [b for j in done for b in blocks_of(j)]
        now = [order[b] for b in blocks_of(i)]
        for s in sorted({s for s in now if all(b in ready for b in (s, 2 * cp - 1 - s))}):
            @pl.when(me_c != s)
            def _():
                pltpu.make_async_remote_copy(out_heads.at[t, pl.ds(s * rows, rows)], outs[t].at[:, mine_at],
                                             out_send.at[t], out_recv.at[t], device_id={"cp": s}, device_id_type=MESH).start()

    def wait_out(t):
        outs[t][:, mine_at] = out_heads[t, my_rows, :]
        pltpu.make_async_copy(others, others, out_recv.at[t]).wait()

    qb = min(256, total)
    blocks = total // qb
    walk = sorted(range(blocks), key=lambda i: -min(i, blocks - 1 - i))

    def causal(shape, q_start, k_start, q_axis):
        q_pos = lax.broadcasted_iota(jnp.int32, shape, q_axis) + q_start
        k_pos = lax.broadcasted_iota(jnp.int32, shape, 1 - q_axis) + k_start
        return q_pos >= k_pos

    for t in range(3):
        wait_in(t)
    for i in walk:
        at, n = pl.ds(i * qb, qb), (i + 1) * qb
        s = mm(sorted_heads[0, at, :], sorted_heads[1, :n, :], NT) * scale
        s = jnp.where(causal(s.shape, i * qb, 0, 0), s, -jnp.inf)
        m = jnp.max(s, axis=1, keepdims=True)
        p = jnp.exp(s - m)
        l = jnp.sum(p, axis=1, keepdims=True)
        o = mm(p.astype(jnp.bfloat16), sorted_heads[2, :n, :]) / l
        o = o.astype(jnp.bfloat16)
        sorted_o[at, :] = o
        put(0, i, o)
        stat[0, at, :] = jnp.broadcast_to(m + jnp.log(l), (qb, hd))
        send_out(0, i)

    wait_in(3)
    for i in range(blocks):
        at = pl.ds(i * qb, qb)
        delta = jnp.sum(sorted_heads[3, at, :].astype(jnp.float32) * sorted_o[at, :].astype(jnp.float32), axis=1, keepdims=True)
        stat[1, at, :] = jnp.broadcast_to(delta, (qb, hd))
    for j in range(2):
        for i in range(total // hd):
            stat_t[j, :, i * hd:(i + 1) * hd] = stat[j, i * hd:(i + 1) * hd, :].T[:8]

    for i in walk:
        at, n = pl.ds(i * qb, qb), (i + 1) * qb
        s = mm(sorted_heads[0, at, :], sorted_heads[1, :n, :], NT) * scale
        p = jnp.where(causal(s.shape, i * qb, 0, 0), jnp.exp(s - stat[0, at, :1]), 0.0)
        dp = mm(sorted_heads[3, at, :], sorted_heads[2, :n, :], NT)
        ds = (p * (dp - stat[1, at, :1])).astype(jnp.bfloat16)
        put(1, i, (mm(ds, sorted_heads[1, :n, :]) * scale).astype(jnp.bfloat16))
        send_out(1, i)
    width = dm // RS_TILES

    def rs_parts(tile, odd):
        onward, back = (left, right) if odd else (right, left)
        at = pl.ds(pl.multiple_of(tile * width, width), width)

        def mine(d):
            return (pl.ds(pl.multiple_of(d * rb, rb), rb), at)

        def copy(src, dst, send, recv, to):
            return pltpu.make_async_remote_copy(src, dst.at[tile], send.at[tile], recv.at[tile],
                                                device_id={"tp": to}, device_id_type=MESH)

        first = lambda: copy(part.at[mine(across)], r1, r1_send, r1_recv, onward)
        second = lambda: copy(s2.at[tile], r2, r2_send, r2_recv, onward)
        direct = lambda: copy(part.at[mine(back)], r3, r3_send, r3_recv, back)
        return at, mine, onward, first, second, direct

    def pairs_of_tiles(step):
        @pl.loop(0, RS_TILES // 2)
        def _(i):
            for odd in range(2):
                step(i * 2 + odd, odd)

    def reduce_first(tile, odd):
        at, _, _, first, _, _ = rs_parts(tile, odd)
        part[:, at] = mm(o_ref[...], wo_all[:, at])
        first().start()

    def reduce_direct(tile, odd):
        rs_parts(tile, odd)[5]().start()

    def reduce_second(tile, odd):
        _, mine, onward, first, second, _ = rs_parts(tile, odd)
        first().wait_recv()
        s2[tile] = r1[tile] + part[mine(onward)]
        second().start()

    def reduce_last(tile, odd):
        at, mine, _, first, second, direct = rs_parts(tile, odd)
        direct().wait_recv()
        second().wait_recv()
        y_ref[:, at] = (part[mine(me_t)] + r2[tile] + r3[tile]).astype(jnp.bfloat16)
        first().wait_send()
        second().wait_send()
        direct().wait_send()

    wait_out(0)
    pairs_of_tiles(reduce_first)
    pairs_of_tiles(reduce_direct)
    for i in walk:
        at, after = pl.ds(i * qb, qb), pl.ds(i * qb, total - i * qb)
        s = mm(sorted_heads[1, at, :], sorted_heads[0, after, :], NT) * scale
        p = jnp.where(causal(s.shape, 0, 0, 1), jnp.exp(s - stat_t[0, :1, after]), 0.0)
        dp = mm(sorted_heads[2, at, :], sorted_heads[3, after, :], NT)
        ds = (p * (dp - stat_t[1, :1, after])).astype(jnp.bfloat16)
        put(3, i, mm(p.astype(jnp.bfloat16), sorted_heads[3, after, :]).astype(jnp.bfloat16))
        send_out(3, i)
        put(2, i, (mm(ds, sorted_heads[0, after, :]) * scale).astype(jnp.bfloat16))
        send_out(2, i)

    pairs_of_tiles(reduce_second)


    def dx_copy(tile, odd):
        spot = (pl.ds(pl.multiple_of(across * rb, rb), rb), pl.ds(pl.multiple_of((tile + odd * RS_TILES // 2) * width, width), width))
        return pltpu.make_async_remote_copy(dx_part.at[spot], r4.at[odd, tile], r4_send.at[odd, tile], r4_recv.at[odd, tile],
                                            device_id={"tp": left if odd else right}, device_id_type=MESH)

    def block_of(d, at):
        return dx_part[pl.ds(pl.multiple_of(d * rb, rb), rb), at]

    def dx_term(t, w, at):
        return mm(outs[t][...], wall[w, at, :], NT)

    for t, w in ((1, 0), (3, 2)):
        wait_out(t)

        @pl.loop(0, RS_TILES)
        def _(i):
            at = pl.ds(pl.multiple_of(i * width, width), width)
            term = dx_term(t, w, at)
            dx_part[:, at] = term if t == 1 else dx_part[:, at] + term

    wait_out(2)

    @pl.loop(0, RS_TILES // 2)
    def _(i):
        for odd, (back_ref, back) in enumerate(((back_l, left), (back_r, right))):
            at = pl.ds(pl.multiple_of((i + odd * RS_TILES // 2) * width, width), width)
            dx_part[:, at] += dx_term(2, 1, at)
            dx_copy(i, odd).start()
            own_ref[:, at] = block_of(me_t, at)
            back_ref[:, pl.ds(pl.multiple_of(i * width, width), width)] = block_of(back, at)

    pairs_of_tiles(reduce_last)

    @pl.loop(0, RS_TILES // 2)
    def _(i):
        for odd, (on_ref, onward) in enumerate(((on_r, right), (on_l, left))):
            at = pl.ds(pl.multiple_of((i + odd * RS_TILES // 2) * width, width), width)
            dx_copy(i, odd).wait_recv()
            on_ref[:, pl.ds(pl.multiple_of(i * width, width), width)] = r4[odd, i] + block_of(onward, at)
            dx_copy(i, odd).wait_send()

    x_copy.wait()
    dy_copy.wait()
    for t in range(4):
        for sem in (in_send, out_send):
            pltpu.make_async_copy(others, others, sem.at[t]).wait()
    for which, src, dst in ((0, x_ref, xr_ref), (1, dy_ref, dyr_ref)):
        for idx, col_half, to in ((0, 0, right), (1, 1, left), (2, 1, right), (3, 0, left)):
            gather_copy(src, dst, which, idx, me_t, col_half, to).wait_send()
        gather_copy(dst, dst, which, 4, left, 0, right).wait_send()
        gather_copy(dst, dst, which, 5, right, 1, left).wait_send()


def attention_call(tp, cp, x_blk, dy_blk, wq, wk, wv, wo):
    rb, dm = x_blk.shape
    rows = rb * tp
    hc, _ = wo.shape
    hd = hc // cp
    total = rows * cp
    bf, f32 = jnp.bfloat16, jnp.float32
    chunk = dm // CHUNKS
    width = dm // RS_TILES
    vmem, hbm = pl.BlockSpec(memory_space=pltpu.VMEM), pl.BlockSpec(memory_space=pl.ANY)
    out = lambda r, c: jax.ShapeDtypeStruct((r, c), bf)
    wide = lambda c: jax.ShapeDtypeStruct((rb, c), f32)
    dma = pltpu.SemaphoreType.DMA
    return pl.pallas_call(
        functools.partial(attention_kernel, tp, cp),
        out_shape=(out(rb, dm), wide(dm), *[wide(dm // 2)] * 4, out(rows, dm), out(rows, dm), out(rows, hc), out(rows, hc), out(rows, hc), out(rows, hc)),
        in_specs=[vmem, vmem, hbm, hbm, hbm, hbm],
        out_specs=[vmem] * 6 + [hbm] * 2 + [vmem] * 4,
        scratch_shapes=[
            pltpu.VMEM((rows, dm), bf), pltpu.VMEM((rows, dm), bf),
            pltpu.VMEM((SLOTS, chunk * cp, hd), bf), pltpu.VMEM((STRIPS, chunk // STRIPS * max(cp, PITCH), hd), f32),
            pltpu.VMEM((3, dm, hc), bf), pltpu.VMEM((hc, dm), bf),
            pltpu.VMEM((4, rows, hc), bf), pltpu.VMEM((4, total, hd), bf),
            pltpu.VMEM((4, total, hd), bf), pltpu.VMEM((total, hd), bf), pltpu.VMEM((4, total, hd), bf),
            pltpu.VMEM((2, total, hd), f32), pltpu.VMEM((2, 8, total), f32),
            pltpu.VMEM((rows, dm), f32), pltpu.VMEM((rows, dm), f32),
            pltpu.VMEM((RS_TILES, rb, width), f32), pltpu.VMEM((RS_TILES, rb, width), f32),
            pltpu.VMEM((RS_TILES, rb, width), f32), pltpu.VMEM((RS_TILES, rb, width), f32),
            pltpu.VMEM((2, RS_TILES // 2, rb, width), f32),
            dma((SLOTS,)), dma, dma((2,)), dma((2, 6)), dma((2, 6)), dma((4,)), dma((4,)), dma((4,)), dma((4,)),
            *[dma((RS_TILES,))] * 6, *[dma((2, RS_TILES // 2))] * 2,
        ],
        compiler_params=pltpu.CompilerParams(collective_id=0, has_side_effects=True, vmem_limit_bytes=VMEM_BYTES),
    )(x_blk, dy_blk, wq, wk, wv, wo)


def grad_kernel(n_heads, x_hbm, dy_hbm, o_hbm, dq_hbm, dk_hbm, dv_hbm, y_ref, gq_ref, gk_ref, gv_ref, go_ref, y_out,
                x_ref, dy_ref, o_ref, dq_ref, dk_ref, dv_ref, wide, grads, out_grad, in_sem, out_sem):
    rows, dm = x_ref.shape
    hd = wide.shape[-1]
    tiles = grads.shape[1]
    m_tile, o_tile = dm // tiles, n_heads * hd // tiles
    pitch = wide.shape[1] // m_tile
    loads = [pltpu.make_async_copy(src, dst, in_sem.at[i]) for i, (src, dst) in enumerate(
        ((dq_hbm, dq_ref), (x_hbm, x_ref), (dk_hbm, dk_ref), (dv_hbm, dv_ref), (o_hbm, o_ref), (dy_hbm, dy_ref)))]
    for load in loads:
        load.start()
    y_out[...] = y_ref[...]
    for load in loads[:4]:
        load.wait()

    @pl.loop(0, tiles)
    def _(i):
        at = pl.ds(pl.multiple_of(i * m_tile, m_tile), m_tile)
        tall = pl.ds(pl.multiple_of(i * m_tile * n_heads, m_tile * n_heads), m_tile * n_heads)
        x_t = x_ref[:, at].T
        for t, (d_ref, g_ref) in enumerate(((dq_ref, gq_ref), (dk_ref, gk_ref), (dv_ref, gv_ref))):
            for h in range(0, n_heads, 2):
                grad = mm(x_t, d_ref[:, h * hd:(h + 2) * hd])
                for e in range(2):
                    wide[t, pl.ds(h + e, m_tile, stride=pitch), :] = grad[:, e * hd:(e + 1) * hd]
            for r in range(0, m_tile, 2):
                pair = jnp.concatenate([wide[t, (r + e) * pitch:(r + e) * pitch + n_heads, :] for e in range(2)], axis=0)
                grads[t, i, r * n_heads:(r + 2) * n_heads, :] = pair.astype(jnp.bfloat16)
            pltpu.make_async_copy(grads.at[t, i], g_ref.at[tall], out_sem.at[t]).start()

    for load in loads[4:]:
        load.wait()

    @pl.loop(0, tiles)
    def _(i):
        at = pl.ds(pl.multiple_of(i * o_tile, o_tile), o_tile)
        out_grad[at, :] = mm(o_ref[:, at], dy_ref[...], TN).astype(jnp.bfloat16)
        pltpu.make_async_copy(out_grad.at[at], go_ref.at[at], out_sem.at[3]).start()

    for t, g_ref in enumerate((gq_ref, gk_ref, gv_ref, go_ref)):
        pltpu.make_async_copy(g_ref, g_ref, out_sem.at[t]).wait()


def grad_call(n_heads, x_rows, dy_rows, o_flat, dq, dk, dv, y_blk):
    rows, dm = x_rows.shape
    hc = o_flat.shape[1]
    hd = hc // n_heads
    tiles = n_heads
    bf, f32 = jnp.bfloat16, jnp.float32
    hbm, vmem = pl.BlockSpec(memory_space=pl.ANY), pl.BlockSpec(memory_space=pltpu.VMEM)
    inputs = (x_rows, dy_rows, o_flat, dq, dk, dv)
    return pl.pallas_call(
        functools.partial(grad_kernel, n_heads),
        out_shape=[jax.ShapeDtypeStruct((dm * n_heads, hd), bf)] * 3 + [jax.ShapeDtypeStruct((hc, dm), bf), jax.ShapeDtypeStruct(y_blk.shape, bf)],
        in_specs=[hbm] * 6 + [vmem],
        out_specs=[hbm] * 4 + [vmem],
        scratch_shapes=[*[pltpu.VMEM(a.shape, bf) for a in inputs],
                        pltpu.VMEM((3, dm // tiles * max(n_heads, PITCH), hd), f32), pltpu.VMEM((3, tiles, dm // tiles * n_heads, hd), bf),
                        pltpu.VMEM((hc, dm), bf), pltpu.SemaphoreType.DMA((6,)), pltpu.SemaphoreType.DMA((4,))],
        compiler_params=pltpu.CompilerParams(vmem_limit_bytes=VMEM_BYTES),
        cost_estimate=pl.CostEstimate(flops=8 * rows * dm * hc, bytes_accessed=8 * dm * hc + 8 * rows * dm, transcendentals=0),
    )(*inputs, y_blk)


def add_kernel(own, direct_a, last_a, direct_b, last_b, dx_ref):
    cols = direct_a.shape[1]
    dx_ref[:, :cols] = (own[:, :cols] + direct_a[...] + last_a[...]).astype(jnp.bfloat16)
    dx_ref[:, cols:] = (own[:, cols:] + direct_b[...] + last_b[...]).astype(jnp.bfloat16)


def solution(mesh):
    tp, cp = mesh.shape["tp"], mesh.shape["cp"]

    def device_fn(x_blk, w_query, w_key, w_value, w_out, dy_blk):
        dm, n_heads, hd = w_query.shape
        if tp != 4 or n_heads != cp or w_key.shape != w_query.shape:
            raise ValueError("unsupported split")
        tall = lambda w: w.reshape(dm * n_heads, hd)
        y_blk, own, back_l, back_r, on_r, on_l, x_rows, dy_rows, o_flat, dq, dk, dv = attention_call(
            tp, cp, x_blk, dy_blk, tall(w_query), tall(w_key), tall(w_value), w_out.reshape(n_heads * hd, dm))
        to_right = lambda a: lax.ppermute(a, "tp", [(i, (i + 1) % tp) for i in range(tp)])
        to_left = lambda a: lax.ppermute(a, "tp", [(i, (i - 1) % tp) for i in range(tp)])
        last_a, last_b, direct_a, direct_b = to_right(on_r), to_left(on_l), to_left(back_l), to_right(back_r)
        gq, gk, gv, go, y_blk = grad_call(n_heads, x_rows, dy_rows, o_flat, dq, dk, dv, y_blk)
        vmem = pl.BlockSpec(memory_space=pltpu.VMEM)
        dx_blk = pl.pallas_call(add_kernel, out_shape=jax.ShapeDtypeStruct(own.shape, jnp.bfloat16), in_specs=[vmem] * 5, out_specs=vmem)(
            own, direct_a, last_a, direct_b, last_b)
        split = lambda g: g.reshape(1, dm, n_heads, hd)
        return y_blk, dx_blk, split(gq), split(gk), split(gv), go.reshape(1, n_heads, hd, dm)

    return jax.shard_map(device_fn, mesh=mesh,
                         in_specs=(ROW_SPEC, HEAD_SPEC, HEAD_SPEC, HEAD_SPEC, OUT_W_SPEC, ROW_SPEC),
                         out_specs=(ROW_SPEC, ROW_SPEC, GRAD_SPEC, GRAD_SPEC, GRAD_SPEC, GRAD_OUT_SPEC),
                         check_vma=False)
```

```python
import functools

import jax
import jax.numpy as jnp
from jax import lax
from jax.experimental import pallas as pl
from jax.experimental.pallas import tpu as pltpu
from jax.sharding import PartitionSpec as P

ROW_SPEC = P(("dp", "cp", "tp"), None)
HEAD_SPEC = P(None, "tp", None)
OUT_W_SPEC = P("tp", None, None)
GRAD_SPEC = P(("dp", "cp"), None, "tp", None)
GRAD_OUT_SPEC = P(("dp", "cp"), "tp", None, None)
NT = (((1,), (1,)), ((), ()))
TN = (((0,), (0,)), ((), ()))
NN = (((1,), (0,)), ((), ()))
MESH = pl.DeviceIdType.MESH
VMEM_BYTES = 67_043_328
RS_TILES = 8
CHUNKS = 16
SLOTS = 8
STRIPS = 4
PITCH = 12


def mm(a, b, dims=NN):
    return lax.dot_general(a, b, dims, preferred_element_type=jnp.float32)


def attention_kernel(tp, cp, *refs):
    (x_hbm, dy_hbm, wq_ref, wk_ref, wv_ref, wo_ref,
     y_ref, own_ref, back_l, back_r, on_r, on_l, x_out, dy_out, o_ref, dq_ref, dk_ref, dv_ref,
     x_ref, dy_ref, xr_ref, dyr_ref, wbuf, wf32, wall, wo_all, flat, heads, relay, sorted_heads, sorted_o, out_heads, stat, stat_t,
     part, dx_part, r1, r2, r3, s2, r4,
     w_sem, wo_sem, load_sem, row_sem, ag_send, ag_recv, in_send, in_recv, relay_send, relay_recv, out_send, out_recv,
     r1_send, r1_recv, r2_send, r2_recv, r3_send, r3_recv, r4_send, r4_recv) = refs
    me_t, me_c = lax.axis_index("tp"), lax.axis_index("cp")
    right, left, across = (me_t + 1) % tp, (me_t + tp - 1) % tp, (me_t + 2) % tp
    rb, dm = x_ref.shape
    rows = rb * tp
    half = rows // 2
    cols = dm // 2
    total, hd = heads.shape[1:]
    n_heads = cp
    scale = hd ** -0.5

    w_refs = (wq_ref, wk_ref, wv_ref)
    others = heads.at[0, pl.ds(0, (cp - 1) * rows)]
    chunk = dm // CHUNKS

    def w_copy(t, c, slot):
        return pltpu.make_async_copy(w_refs[t].at[pl.ds(c * chunk * n_heads, chunk * n_heads)], wbuf.at[slot], w_sem.at[slot])

    loads = [pltpu.make_async_copy(src, dst, load_sem.at[i]) for i, (src, dst) in enumerate(((x_hbm, x_ref), (dy_hbm, dy_ref)))]
    for load in loads:
        load.start()
    for c in range(SLOTS):
        w_copy(0, c, c).start()

    barrier = pltpu.get_barrier_semaphore()
    for t_dev in (left, right):
        pl.semaphore_signal(barrier, inc=1, device_id={"tp": t_dev}, device_id_type=MESH)
    for k in range(1, cp):
        pl.semaphore_signal(barrier, inc=1, device_id={"cp": (me_c + k) % cp}, device_id_type=MESH)
    pl.semaphore_wait(barrier, 2 + cp - 1)

    def gather_copy(src, dst, which, idx, block, col_half, to):
        where = (pl.ds(block * rb, rb), pl.ds(col_half * cols, cols))
        src_view = src.at[:, pl.ds(col_half * cols, cols)] if src is not dst else dst.at[where]
        return pltpu.make_async_remote_copy(src_view, dst.at[where], ag_send.at[which, idx], ag_recv.at[which, idx],
                                            device_id={"tp": to}, device_id_type=MESH)

    def gather_start(which, src, dst):
        for idx, col_half, to in ((0, 0, right), (1, 1, left), (2, 1, right), (3, 0, left)):
            gather_copy(src, dst, which, idx, me_t, col_half, to).start()
        dst[pl.ds(pl.multiple_of(me_t * rb, rb), rb), :] = src[...]

    def gather_pass(which, src, dst):
        gather_copy(src, dst, which, 0, left, 0, right).wait_recv()
        gather_copy(dst, dst, which, 4, left, 0, right).start()
        gather_copy(src, dst, which, 1, right, 1, left).wait_recv()
        gather_copy(dst, dst, which, 5, right, 1, left).start()

    def gather_end(which, src, dst):
        gather_copy(src, dst, which, 2, left, 1, right).wait_recv()
        gather_copy(src, dst, which, 3, right, 0, left).wait_recv()
        gather_copy(dst, dst, which, 4, across, 0, right).wait_recv()
        gather_copy(dst, dst, which, 5, across, 1, left).wait_recv()

    pitch = wf32.shape[1] // (chunk // STRIPS)

    def relayout(t):
        @pl.loop(0, CHUNKS)
        def _(c):
            slot = c % SLOTS
            w_copy(t, c, slot).wait()
            strip = chunk // STRIPS
            for k in range(STRIPS + 1):
                if k < STRIPS:
                    for r in range(0, strip, 2):
                        at = (k * strip + r) * n_heads
                        pair = wbuf[slot, at:at + 2 * n_heads].astype(jnp.float32)
                        for e in range(2):
                            wf32[k, (r + e) * pitch:(r + e) * pitch + n_heads] = pair[e * n_heads:(e + 1) * n_heads]
                if k > 0:
                    at = pl.ds(pl.multiple_of(c * chunk + (k - 1) * strip, strip), strip)
                    for h in range(n_heads):
                        wall[t, at, h * hd:(h + 1) * hd] = wf32[k - 1, pl.ds(h, strip, stride=pitch), :].astype(jnp.bfloat16)

            @pl.when(c + SLOTS < CHUNKS)
            def _():
                w_copy(t, c + SLOTS, slot).start()

            if t + 1 < len(w_refs):
                @pl.when(c + SLOTS >= CHUNKS)
                def _():
                    w_copy(t + 1, c + SLOTS - CHUNKS, slot).start()

    for load in loads:
        load.wait()
    gather_start(0, x_ref, xr_ref)
    relayout(0)
    gather_pass(0, x_ref, xr_ref)
    gather_start(1, dy_ref, dyr_ref)
    relayout(1)
    wo_copy = pltpu.make_async_copy(wo_ref, wo_all, wo_sem)
    wo_copy.start()
    relayout(2)
    gather_end(0, x_ref, xr_ref)
    x_copy = pltpu.make_async_copy(xr_ref, x_out, row_sem.at[0])
    x_copy.start()
    gather_pass(1, dy_ref, dyr_ref)

    mine_at = pl.ds(pl.multiple_of(me_c * hd, hd), hd)
    my_rows = pl.ds(pl.multiple_of(me_c * rows, rows), rows)

    def send_in(t, h):
        @pl.when(h != me_c)
        def _():
            pltpu.make_async_remote_copy(flat.at[t, :, pl.ds(pl.multiple_of(h * hd, hd), hd)], heads.at[t, my_rows],
                                         in_send.at[t], in_recv.at[t], device_id={"cp": h}, device_id_type=MESH).start()

    order = [s if s < cp else 2 * cp - 1 - s for s in range(2 * cp)]

    def wait_in(t):
        pltpu.make_async_copy(others, others, in_recv.at[t]).wait()
        heads[t, my_rows, :] = flat[t, :, mine_at]
        for b, s in enumerate(order):
            start = s * rows + (half if b >= cp else 0)
            sorted_heads[t, b * half:(b + 1) * half, :] = heads[t, start:start + half, :]

    pairs = cp // 2
    chip, core = me_c // 2, me_c % 2
    ways = ((1, 0), (pairs - 1, half)) if pairs == 4 else ()

    def relay_start(t):
        for d, (step, start) in enumerate(ways):
            far = pl.ds(pl.multiple_of((chip + 2) % pairs * 2 * hd, 2 * hd), 2 * hd)
            pltpu.make_async_remote_copy(flat.at[t, pl.ds(start, half), far], relay.at[t, d], relay_send.at[t, d], relay_recv.at[t, d],
                                         device_id={"cp": (chip + step) % pairs * 2 + core}, device_id_type=MESH).start()

    def relay_wait(t, d, sem):
        pltpu.make_async_copy(relay.at[t, d], relay.at[t, d], sem.at[t, d]).wait()

    def relay_pass(t):
        for d, (step, start) in enumerate(ways):
            relay_wait(t, d, relay_recv)
            source = (chip + pairs - step) % pairs * 2 + core
            for e in range(2):
                pltpu.make_async_remote_copy(relay.at[t, d, :, pl.ds(e * hd, hd)],
                                             heads.at[t, pl.ds(pl.multiple_of(source * rows + start, half), half)],
                                             in_send.at[t], in_recv.at[t],
                                             device_id={"cp": (chip + step) % pairs * 2 + e}, device_id_type=MESH).start()

    def project(t, compute):
        @pl.loop(0, pairs)
        def _(i):
            pair = (chip + pairs // 2 + i) % pairs
            at = pl.ds(pl.multiple_of(pair * 2 * hd, 2 * hd), 2 * hd)
            flat[t, :, at] = compute(at).astype(jnp.bfloat16)

            def direct():
                for e in range(2):
                    send_in(t, pair * 2 + e)

            if ways:
                pl.when(i == 0)(lambda: relay_start(t))
                pl.when(i != 0)(direct)
            else:
                direct()

    @pl.loop(0, 3)
    def _(t):
        project(t, lambda at: mm(xr_ref[...], wall[t, :, at]))
        relay_pass(t)

    gather_end(1, dy_ref, dyr_ref)
    dy_copy = pltpu.make_async_copy(dyr_ref, dy_out, row_sem.at[1])
    dy_copy.start()
    wo_copy.wait()
    project(3, lambda at: mm(dyr_ref[...], wo_all[at, :], NT))

    outs = (o_ref, dq_ref, dk_ref, dv_ref)

    def put(t, i, value):
        for k in range(qb // half):
            b = i * (qb // half) + k
            start = order[b] * rows + (half if b >= cp else 0)
            out_heads[t, start:start + half, :] = value[k * half:(k + 1) * half]

    def send_out(t, i):
        done = walk[:walk.index(i) + 1]
        blocks_of = lambda i: range(i * (qb // half), (i + 1) * (qb // half))
        ready = [b for j in done for b in blocks_of(j)]
        now = [order[b] for b in blocks_of(i)]
        for s in sorted({s for s in now if all(b in ready for b in (s, 2 * cp - 1 - s))}):
            @pl.when(me_c != s)
            def _():
                pltpu.make_async_remote_copy(out_heads.at[t, pl.ds(s * rows, rows)], outs[t].at[:, mine_at],
                                             out_send.at[t], out_recv.at[t], device_id={"cp": s}, device_id_type=MESH).start()

    def wait_out(t):
        outs[t][:, mine_at] = out_heads[t, my_rows, :]
        pltpu.make_async_copy(others, others, out_recv.at[t]).wait()

    qb = min(256, total)
    blocks = total // qb
    walk = sorted(range(blocks), key=lambda i: -min(i, blocks - 1 - i))

    def causal(shape, q_start, k_start, q_axis):
        q_pos = lax.broadcasted_iota(jnp.int32, shape, q_axis) + q_start
        k_pos = lax.broadcasted_iota(jnp.int32, shape, 1 - q_axis) + k_start
        return q_pos >= k_pos

    for t in range(3):
        wait_in(t)
    for i in walk:
        at, n = pl.ds(i * qb, qb), (i + 1) * qb
        s = mm(sorted_heads[0, at, :], sorted_heads[1, :n, :], NT) * scale
        s = jnp.where(causal(s.shape, i * qb, 0, 0), s, -jnp.inf)
        m = jnp.max(s, axis=1, keepdims=True)
        p = jnp.exp(s - m)
        l = jnp.sum(p, axis=1, keepdims=True)
        o = mm(p.astype(jnp.bfloat16), sorted_heads[2, :n, :]) / l
        o = o.astype(jnp.bfloat16)
        sorted_o[at, :] = o
        put(0, i, o)
        stat[0, at, :] = jnp.broadcast_to(m + jnp.log(l), (qb, hd))
        send_out(0, i)

    relay_pass(3)
    wait_in(3)
    for i in range(blocks):
        at = pl.ds(i * qb, qb)
        delta = jnp.sum(sorted_heads[3, at, :].astype(jnp.float32) * sorted_o[at, :].astype(jnp.float32), axis=1, keepdims=True)
        stat[1, at, :] = jnp.broadcast_to(delta, (qb, hd))
    for j in range(2):
        for i in range(total // hd):
            stat_t[j, :, i * hd:(i + 1) * hd] = stat[j, i * hd:(i + 1) * hd, :].T[:8]

    for i in walk:
        at, n = pl.ds(i * qb, qb), (i + 1) * qb
        s = mm(sorted_heads[0, at, :], sorted_heads[1, :n, :], NT) * scale
        p = jnp.where(causal(s.shape, i * qb, 0, 0), jnp.exp(s - stat[0, at, :1]), 0.0)
        dp = mm(sorted_heads[3, at, :], sorted_heads[2, :n, :], NT)
        ds = (p * (dp - stat[1, at, :1])).astype(jnp.bfloat16)
        put(1, i, (mm(ds, sorted_heads[1, :n, :]) * scale).astype(jnp.bfloat16))
        send_out(1, i)
    width = dm // RS_TILES

    def rs_parts(tile, odd):
        onward, back = (left, right) if odd else (right, left)
        at = pl.ds(pl.multiple_of(tile * width, width), width)

        def mine(d):
            return (pl.ds(pl.multiple_of(d * rb, rb), rb), at)

        def copy(src, dst, send, recv, to):
            return pltpu.make_async_remote_copy(src, dst.at[tile], send.at[tile], recv.at[tile],
                                                device_id={"tp": to}, device_id_type=MESH)

        first = lambda: copy(part.at[mine(across)], r1, r1_send, r1_recv, onward)
        second = lambda: copy(s2.at[tile], r2, r2_send, r2_recv, onward)
        direct = lambda: copy(part.at[mine(back)], r3, r3_send, r3_recv, back)
        return at, mine, onward, first, second, direct

    def pairs_of_tiles(step):
        @pl.loop(0, RS_TILES // 2)
        def _(i):
            for odd in range(2):
                step(i * 2 + odd, odd)

    def reduce_first(tile, odd):
        at, _, _, first, _, _ = rs_parts(tile, odd)
        part[:, at] = mm(o_ref[...], wo_all[:, at])
        first().start()

    def reduce_direct(tile, odd):
        rs_parts(tile, odd)[5]().start()

    def reduce_second(tile, odd):
        _, mine, onward, first, second, _ = rs_parts(tile, odd)
        first().wait_recv()
        s2[tile] = r1[tile] + part[mine(onward)]
        second().start()

    def reduce_last(tile, odd):
        at, mine, _, first, second, direct = rs_parts(tile, odd)
        direct().wait_recv()
        second().wait_recv()
        y_ref[:, at] = (part[mine(me_t)] + r2[tile] + r3[tile]).astype(jnp.bfloat16)
        first().wait_send()
        second().wait_send()
        direct().wait_send()

    wait_out(0)
    pairs_of_tiles(reduce_first)
    pairs_of_tiles(reduce_direct)
    for i in walk:
        at, after = pl.ds(i * qb, qb), pl.ds(i * qb, total - i * qb)
        s = mm(sorted_heads[1, at, :], sorted_heads[0, after, :], NT) * scale
        p = jnp.where(causal(s.shape, 0, 0, 1), jnp.exp(s - stat_t[0, :1, after]), 0.0)
        dp = mm(sorted_heads[2, at, :], sorted_heads[3, after, :], NT)
        ds = (p * (dp - stat_t[1, :1, after])).astype(jnp.bfloat16)
        put(3, i, mm(p.astype(jnp.bfloat16), sorted_heads[3, after, :]).astype(jnp.bfloat16))
        send_out(3, i)
        put(2, i, (mm(ds, sorted_heads[0, after, :]) * scale).astype(jnp.bfloat16))
        send_out(2, i)

    pairs_of_tiles(reduce_second)


    def dx_copy(tile, odd):
        spot = (pl.ds(pl.multiple_of(across * rb, rb), rb), pl.ds(pl.multiple_of((tile + odd * RS_TILES // 2) * width, width), width))
        return pltpu.make_async_remote_copy(dx_part.at[spot], r4.at[odd, tile], r4_send.at[odd, tile], r4_recv.at[odd, tile],
                                            device_id={"tp": left if odd else right}, device_id_type=MESH)

    def block_of(d, at):
        return dx_part[pl.ds(pl.multiple_of(d * rb, rb), rb), at]

    def dx_term(t, w, at):
        return mm(outs[t][...], wall[w, at, :], NT)

    for t, w in ((1, 0), (3, 2)):
        wait_out(t)

        @pl.loop(0, RS_TILES)
        def _(i):
            at = pl.ds(pl.multiple_of(i * width, width), width)
            term = dx_term(t, w, at)
            dx_part[:, at] = term if t == 1 else dx_part[:, at] + term

    wait_out(2)

    @pl.loop(0, RS_TILES // 2)
    def _(i):
        for odd, (back_ref, back) in enumerate(((back_l, left), (back_r, right))):
            at = pl.ds(pl.multiple_of((i + odd * RS_TILES // 2) * width, width), width)
            dx_part[:, at] += dx_term(2, 1, at)
            dx_copy(i, odd).start()
            own_ref[:, at] = block_of(me_t, at)
            back_ref[:, pl.ds(pl.multiple_of(i * width, width), width)] = block_of(back, at)

    pairs_of_tiles(reduce_last)

    @pl.loop(0, RS_TILES // 2)
    def _(i):
        for odd, (on_ref, onward) in enumerate(((on_r, right), (on_l, left))):
            at = pl.ds(pl.multiple_of((i + odd * RS_TILES // 2) * width, width), width)
            dx_copy(i, odd).wait_recv()
            on_ref[:, pl.ds(pl.multiple_of(i * width, width), width)] = r4[odd, i] + block_of(onward, at)
            dx_copy(i, odd).wait_send()

    x_copy.wait()
    dy_copy.wait()
    for t in range(4):
        for d in range(len(ways)):
            relay_wait(t, d, relay_send)
        for sem in (in_send, out_send):
            pltpu.make_async_copy(others, others, sem.at[t]).wait()
    for which, src, dst in ((0, x_ref, xr_ref), (1, dy_ref, dyr_ref)):
        for idx, col_half, to in ((0, 0, right), (1, 1, left), (2, 1, right), (3, 0, left)):
            gather_copy(src, dst, which, idx, me_t, col_half, to).wait_send()
        gather_copy(dst, dst, which, 4, left, 0, right).wait_send()
        gather_copy(dst, dst, which, 5, right, 1, left).wait_send()


def attention_call(tp, cp, x_blk, dy_blk, wq, wk, wv, wo):
    rb, dm = x_blk.shape
    rows = rb * tp
    hc, _ = wo.shape
    hd = hc // cp
    total = rows * cp
    bf, f32 = jnp.bfloat16, jnp.float32
    chunk = dm // CHUNKS
    width = dm // RS_TILES
    vmem, hbm = pl.BlockSpec(memory_space=pltpu.VMEM), pl.BlockSpec(memory_space=pl.ANY)
    out = lambda r, c: jax.ShapeDtypeStruct((r, c), bf)
    wide = lambda c: jax.ShapeDtypeStruct((rb, c), f32)
    dma = pltpu.SemaphoreType.DMA
    return pl.pallas_call(
        functools.partial(attention_kernel, tp, cp),
        out_shape=(out(rb, dm), wide(dm), *[wide(dm // 2)] * 4, out(rows, dm), out(rows, dm), out(rows, hc), out(rows, hc), out(rows, hc), out(rows, hc)),
        in_specs=[hbm] * 6,
        out_specs=[vmem] * 6 + [hbm] * 2 + [vmem] * 4,
        scratch_shapes=[
            pltpu.VMEM((rb, dm), bf), pltpu.VMEM((rb, dm), bf), pltpu.VMEM((rows, dm), bf), pltpu.VMEM((rows, dm), bf),
            pltpu.VMEM((SLOTS, chunk * cp, hd), bf), pltpu.VMEM((STRIPS, chunk // STRIPS * max(cp, PITCH), hd), f32),
            pltpu.VMEM((3, dm, hc), bf), pltpu.VMEM((hc, dm), bf),
            pltpu.VMEM((4, rows, hc), bf), pltpu.VMEM((4, total, hd), bf), pltpu.VMEM((4, 2, rows // 2, 2 * hd), bf),
            pltpu.VMEM((4, total, hd), bf), pltpu.VMEM((total, hd), bf), pltpu.VMEM((4, total, hd), bf),
            pltpu.VMEM((2, total, hd), f32), pltpu.VMEM((2, 8, total), f32),
            pltpu.VMEM((rows, dm), f32), pltpu.VMEM((rows, dm), f32),
            pltpu.VMEM((RS_TILES, rb, width), f32), pltpu.VMEM((RS_TILES, rb, width), f32),
            pltpu.VMEM((RS_TILES, rb, width), f32), pltpu.VMEM((RS_TILES, rb, width), f32),
            pltpu.VMEM((2, RS_TILES // 2, rb, width), f32),
            dma((SLOTS,)), dma, dma((2,)), dma((2,)), dma((2, 6)), dma((2, 6)), dma((4,)), dma((4,)), dma((4, 2)), dma((4, 2)), dma((4,)), dma((4,)),
            *[dma((RS_TILES,))] * 6, *[dma((2, RS_TILES // 2))] * 2,
        ],
        compiler_params=pltpu.CompilerParams(collective_id=0, has_side_effects=True, vmem_limit_bytes=VMEM_BYTES),
    )(x_blk, dy_blk, wq, wk, wv, wo)


def grad_kernel(n_heads, x_hbm, dy_hbm, o_hbm, dq_hbm, dk_hbm, dv_hbm, y_hbm, gq_ref, gk_ref, gv_ref, go_ref, y_out,
                x_ref, dy_ref, o_ref, dq_ref, dk_ref, dv_ref, y_ref, wide, grads, out_grad, in_sem, out_sem):
    rows, dm = x_ref.shape
    hd = wide.shape[-1]
    tiles = grads.shape[1]
    m_tile = dm // tiles
    pitch = wide.shape[1] // m_tile
    loads = [pltpu.make_async_copy(src, dst, in_sem.at[i]) for i, (src, dst) in enumerate(
        ((dq_hbm, dq_ref), (x_hbm, x_ref), (dk_hbm, dk_ref), (dv_hbm, dv_ref), (o_hbm, o_ref), (dy_hbm, dy_ref), (y_hbm, y_ref)))]
    for load in loads:
        load.start()
    for load in loads[:4]:
        load.wait()

    @pl.loop(0, tiles)
    def _(i):
        at = pl.ds(pl.multiple_of(i * m_tile, m_tile), m_tile)
        tall = pl.ds(pl.multiple_of(i * m_tile * n_heads, m_tile * n_heads), m_tile * n_heads)
        x_t = x_ref[:, at].T
        for t, (d_ref, g_ref) in enumerate(((dq_ref, gq_ref), (dk_ref, gk_ref), (dv_ref, gv_ref))):
            for h in range(0, n_heads, 2):
                grad = mm(x_t, d_ref[:, h * hd:(h + 2) * hd])
                for e in range(2):
                    wide[t, pl.ds(h + e, m_tile, stride=pitch), :] = grad[:, e * hd:(e + 1) * hd]
            for r in range(0, m_tile, 2):
                pair = jnp.concatenate([wide[t, (r + e) * pitch:(r + e) * pitch + n_heads, :] for e in range(2)], axis=0)
                grads[t, i, r * n_heads:(r + 2) * n_heads, :] = pair.astype(jnp.bfloat16)
            pltpu.make_async_copy(grads.at[t, i], g_ref.at[tall], out_sem.at[t]).start()

    for load in loads[4:]:
        load.wait()
    y_out_copy = pltpu.make_async_copy(y_ref, y_out, out_sem.at[4])
    y_out_copy.start()

    o_rows, o_cols = out_grad.shape[1:]
    across = dm // o_cols

    @pl.loop(0, out_grad.shape[0])
    def _(i):
        r, c = pl.multiple_of(i // across * o_rows, o_rows), pl.multiple_of(i % across * o_cols, o_cols)
        out_grad[i] = mm(o_ref[:, pl.ds(r, o_rows)], dy_ref[:, pl.ds(c, o_cols)], TN).astype(jnp.bfloat16)
        pltpu.make_async_copy(out_grad.at[i], go_ref.at[pl.ds(r, o_rows), pl.ds(c, o_cols)], out_sem.at[3]).start()

    y_out_copy.wait()
    for t, g_ref in enumerate((gq_ref, gk_ref, gv_ref, go_ref)):
        pltpu.make_async_copy(g_ref, g_ref, out_sem.at[t]).wait()


def grad_call(n_heads, x_rows, dy_rows, o_flat, dq, dk, dv, y_blk):
    rows, dm = x_rows.shape
    hc = o_flat.shape[1]
    hd = hc // n_heads
    tiles = n_heads
    bf, f32 = jnp.bfloat16, jnp.float32
    hbm = pl.BlockSpec(memory_space=pl.ANY)
    inputs = (x_rows, dy_rows, o_flat, dq, dk, dv, y_blk)
    o_rows, o_cols = hc // 2, dm // 4
    return pl.pallas_call(
        functools.partial(grad_kernel, n_heads),
        out_shape=[jax.ShapeDtypeStruct((dm * n_heads, hd), bf)] * 3 + [jax.ShapeDtypeStruct((hc, dm), bf), jax.ShapeDtypeStruct(y_blk.shape, bf)],
        in_specs=[hbm] * 7,
        out_specs=[hbm] * 5,
        scratch_shapes=[*[pltpu.VMEM(a.shape, bf) for a in inputs],
                        pltpu.VMEM((3, dm // tiles * max(n_heads, PITCH), hd), f32), pltpu.VMEM((3, tiles, dm // tiles * n_heads, hd), bf),
                        pltpu.VMEM((8, o_rows, o_cols), bf), pltpu.SemaphoreType.DMA((7,)), pltpu.SemaphoreType.DMA((5,))],
        compiler_params=pltpu.CompilerParams(vmem_limit_bytes=VMEM_BYTES),
        cost_estimate=pl.CostEstimate(flops=8 * rows * dm * hc, bytes_accessed=8 * dm * hc + 8 * rows * dm, transcendentals=0),
    )(*inputs)


def add_kernel(own, direct_a, last_a, direct_b, last_b, dx_ref):
    cols = direct_a.shape[1]
    dx_ref[:, :cols] = (own[:, :cols] + direct_a[...] + last_a[...]).astype(jnp.bfloat16)
    dx_ref[:, cols:] = (own[:, cols:] + direct_b[...] + last_b[...]).astype(jnp.bfloat16)


def solution(mesh):
    tp, cp = mesh.shape["tp"], mesh.shape["cp"]

    def device_fn(x_blk, w_query, w_key, w_value, w_out, dy_blk):
        dm, n_heads, hd = w_query.shape
        if tp != 4 or n_heads != cp or w_key.shape != w_query.shape:
            raise ValueError("unsupported split")
        tall = lambda w: w.reshape(dm * n_heads, hd)
        y_blk, own, back_l, back_r, on_r, on_l, x_rows, dy_rows, o_flat, dq, dk, dv = attention_call(
            tp, cp, x_blk, dy_blk, tall(w_query), tall(w_key), tall(w_value), w_out.reshape(n_heads * hd, dm))
        to_right = lambda a: lax.ppermute(a, "tp", [(i, (i + 1) % tp) for i in range(tp)])
        to_left = lambda a: lax.ppermute(a, "tp", [(i, (i - 1) % tp) for i in range(tp)])
        last_a, last_b, direct_a, direct_b = to_right(on_r), to_left(on_l), to_left(back_l), to_right(back_r)
        gq, gk, gv, go, y_blk = grad_call(n_heads, x_rows, dy_rows, o_flat, dq, dk, dv, y_blk)
        vmem = pl.BlockSpec(memory_space=pltpu.VMEM)
        dx_blk = pl.pallas_call(add_kernel, out_shape=jax.ShapeDtypeStruct(own.shape, jnp.bfloat16), in_specs=[vmem] * 5, out_specs=vmem)(
            own, direct_a, last_a, direct_b, last_b)
        split = lambda g: g.reshape(1, dm, n_heads, hd)
        return y_blk, dx_blk, split(gq), split(gk), split(gv), go.reshape(1, n_heads, hd, dm)

    return jax.shard_map(device_fn, mesh=mesh,
                         in_specs=(ROW_SPEC, HEAD_SPEC, HEAD_SPEC, HEAD_SPEC, OUT_W_SPEC, ROW_SPEC),
                         out_specs=(ROW_SPEC, ROW_SPEC, GRAD_SPEC, GRAD_SPEC, GRAD_SPEC, GRAD_OUT_SPEC),
                         check_vma=False)
```

```python
import functools

import jax
import jax.numpy as jnp
from jax import lax
from jax.experimental import pallas as pl
from jax.experimental.pallas import tpu as pltpu
from jax.sharding import PartitionSpec as P

ROW_SPEC = P(("dp", "cp", "tp"), None)
HEAD_SPEC = P(None, "tp", None)
OUT_W_SPEC = P("tp", None, None)
GRAD_SPEC = P(("dp", "cp"), None, "tp", None)
GRAD_OUT_SPEC = P(("dp", "cp"), "tp", None, None)
NT = (((1,), (1,)), ((), ()))
TN = (((0,), (0,)), ((), ()))
NN = (((1,), (0,)), ((), ()))
MESH = pl.DeviceIdType.MESH
VMEM_BYTES = 67_043_328
RS_TILES = 8
CHUNKS = 16
SLOTS = 8
STRIPS = 4
PITCH = 12


def mm(a, b, dims=NN):
    return lax.dot_general(a, b, dims, preferred_element_type=jnp.float32)


def attention_kernel(tp, cp, *refs):
    (x_hbm, dy_hbm, wq_ref, wk_ref, wv_ref, wo_ref,
     y_ref, own_ref, back_l, back_r, on_r, on_l, x_out, dy_out, o_ref, dq_ref, dk_ref, dv_ref,
     x_ref, dy_ref, xr_ref, dyr_ref, wbuf, wf32, wall, wo_all, flat, heads, sorted_heads, sorted_o, out_heads, stat, stat_t,
     part, dx_part, r1, r2, r3, s2, r4,
     w_sem, wo_sem, load_sem, row_sem, ag_send, ag_recv, in_send, in_recv, out_send, out_recv,
     r1_send, r1_recv, r2_send, r2_recv, r3_send, r3_recv, r4_send, r4_recv) = refs
    me_t, me_c = lax.axis_index("tp"), lax.axis_index("cp")
    right, left, across = (me_t + 1) % tp, (me_t + tp - 1) % tp, (me_t + 2) % tp
    rb, dm = x_ref.shape
    rows = rb * tp
    half = rows // 2
    cols = dm // 2
    total, hd = heads.shape[1:]
    n_heads = cp
    scale = hd ** -0.5

    w_refs = (wq_ref, wk_ref, wv_ref)
    others = heads.at[0, pl.ds(0, (cp - 1) * rows)]
    chunk = dm // CHUNKS

    def w_copy(t, c, slot):
        return pltpu.make_async_copy(w_refs[t].at[pl.ds(c * chunk * n_heads, chunk * n_heads)], wbuf.at[slot], w_sem.at[slot])

    loads = [pltpu.make_async_copy(src, dst, load_sem.at[i]) for i, (src, dst) in enumerate(((x_hbm, x_ref), (dy_hbm, dy_ref)))]
    for load in loads:
        load.start()
    for c in range(SLOTS):
        w_copy(0, c, c).start()

    barrier = pltpu.get_barrier_semaphore()
    for t_dev in (left, right):
        pl.semaphore_signal(barrier, inc=1, device_id={"tp": t_dev}, device_id_type=MESH)
    for k in range(1, cp):
        pl.semaphore_signal(barrier, inc=1, device_id={"cp": (me_c + k) % cp}, device_id_type=MESH)
    pl.semaphore_wait(barrier, 2 + cp - 1)

    def gather_copy(src, dst, which, idx, block, col_half, to):
        where = (pl.ds(block * rb, rb), pl.ds(col_half * cols, cols))
        src_view = src.at[:, pl.ds(col_half * cols, cols)] if src is not dst else dst.at[where]
        return pltpu.make_async_remote_copy(src_view, dst.at[where], ag_send.at[which, idx], ag_recv.at[which, idx],
                                            device_id={"tp": to}, device_id_type=MESH)

    def gather_start(which, src, dst):
        for idx, col_half, to in ((0, 0, right), (1, 1, left), (2, 1, right), (3, 0, left)):
            gather_copy(src, dst, which, idx, me_t, col_half, to).start()
        dst[pl.ds(pl.multiple_of(me_t * rb, rb), rb), :] = src[...]

    def gather_pass(which, src, dst):
        gather_copy(src, dst, which, 0, left, 0, right).wait_recv()
        gather_copy(dst, dst, which, 4, left, 0, right).start()
        gather_copy(src, dst, which, 1, right, 1, left).wait_recv()
        gather_copy(dst, dst, which, 5, right, 1, left).start()

    def gather_end(which, src, dst):
        gather_copy(src, dst, which, 2, left, 1, right).wait_recv()
        gather_copy(src, dst, which, 3, right, 0, left).wait_recv()
        gather_copy(dst, dst, which, 4, across, 0, right).wait_recv()
        gather_copy(dst, dst, which, 5, across, 1, left).wait_recv()

    pitch = wf32.shape[1] // (chunk // STRIPS)

    def relayout(t):
        @pl.loop(0, CHUNKS)
        def _(c):
            slot = c % SLOTS
            w_copy(t, c, slot).wait()
            strip = chunk // STRIPS
            for k in range(STRIPS + 1):
                if k < STRIPS:
                    for r in range(0, strip, 2):
                        at = (k * strip + r) * n_heads
                        pair = wbuf[slot, at:at + 2 * n_heads].astype(jnp.float32)
                        for e in range(2):
                            wf32[k, (r + e) * pitch:(r + e) * pitch + n_heads] = pair[e * n_heads:(e + 1) * n_heads]
                if k > 0:
                    at = pl.ds(pl.multiple_of(c * chunk + (k - 1) * strip, strip), strip)
                    for h in range(n_heads):
                        wall[t, at, h * hd:(h + 1) * hd] = wf32[k - 1, pl.ds(h, strip, stride=pitch), :].astype(jnp.bfloat16)

            @pl.when(c + SLOTS < CHUNKS)
            def _():
                w_copy(t, c + SLOTS, slot).start()

            if t + 1 < len(w_refs):
                @pl.when(c + SLOTS >= CHUNKS)
                def _():
                    w_copy(t + 1, c + SLOTS - CHUNKS, slot).start()

    for load in loads:
        load.wait()
    gather_start(0, x_ref, xr_ref)
    relayout(0)
    gather_pass(0, x_ref, xr_ref)
    gather_start(1, dy_ref, dyr_ref)
    relayout(1)
    wo_copy = pltpu.make_async_copy(wo_ref, wo_all, wo_sem)
    wo_copy.start()
    relayout(2)
    gather_end(0, x_ref, xr_ref)
    x_copy = pltpu.make_async_copy(xr_ref, x_out, row_sem.at[0])
    x_copy.start()

    mine_at = pl.ds(pl.multiple_of(me_c * hd, hd), hd)
    my_rows = pl.ds(pl.multiple_of(me_c * rows, rows), rows)

    def send_in(t, h):
        @pl.when(h != me_c)
        def _():
            pltpu.make_async_remote_copy(flat.at[t, :, pl.ds(pl.multiple_of(h * hd, hd), hd)], heads.at[t, my_rows],
                                         in_send.at[t], in_recv.at[t], device_id={"cp": h}, device_id_type=MESH).start()

    order = [s if s < cp else 2 * cp - 1 - s for s in range(2 * cp)]

    def wait_in(t):
        pltpu.make_async_copy(others, others, in_recv.at[t]).wait()
        heads[t, my_rows, :] = flat[t, :, mine_at]
        for b, s in enumerate(order):
            start = s * rows + (half if b >= cp else 0)
            sorted_heads[t, b * half:(b + 1) * half, :] = heads[t, start:start + half, :]

    pairs = cp // 2
    chip = me_c // 2

    def project(t, compute):
        @pl.loop(0, pairs)
        def _(i):
            pair = (chip + 1 + i) % pairs
            at = pl.ds(pl.multiple_of(pair * 2 * hd, 2 * hd), 2 * hd)
            flat[t, :, at] = compute(at).astype(jnp.bfloat16)
            for e in range(2):
                send_in(t, pair * 2 + e)

    project(0, lambda at: mm(xr_ref[...], wall[0, :, at]))
    gather_pass(1, dy_ref, dyr_ref)
    for t in range(1, 3):
        project(t, lambda at: mm(xr_ref[...], wall[t, :, at]))

    outs = (o_ref, dq_ref, dk_ref, dv_ref)

    def put(t, i, value):
        for k in range(qb // half):
            b = i * (qb // half) + k
            start = order[b] * rows + (half if b >= cp else 0)
            out_heads[t, start:start + half, :] = value[k * half:(k + 1) * half]

    def send_out(t, i):
        done = walk[:walk.index(i) + 1]
        blocks_of = lambda i: range(i * (qb // half), (i + 1) * (qb // half))
        ready = [b for j in done for b in blocks_of(j)]
        now = [order[b] for b in blocks_of(i)]
        for s in sorted({s for s in now if all(b in ready for b in (s, 2 * cp - 1 - s))}):
            @pl.when(me_c != s)
            def _():
                pltpu.make_async_remote_copy(out_heads.at[t, pl.ds(s * rows, rows)], outs[t].at[:, mine_at],
                                             out_send.at[t], out_recv.at[t], device_id={"cp": s}, device_id_type=MESH).start()

    def wait_out(t):
        outs[t][:, mine_at] = out_heads[t, my_rows, :]
        pltpu.make_async_copy(others, others, out_recv.at[t]).wait()

    qb = min(256, total)
    blocks = total // qb
    walk = sorted(range(blocks), key=lambda i: -min(i, blocks - 1 - i))

    def causal(shape, q_start, k_start, q_axis):
        q_pos = lax.broadcasted_iota(jnp.int32, shape, q_axis) + q_start
        k_pos = lax.broadcasted_iota(jnp.int32, shape, 1 - q_axis) + k_start
        return q_pos >= k_pos

    for t in range(3):
        wait_in(t)
    for i in walk:
        at, n = pl.ds(i * qb, qb), (i + 1) * qb
        s = mm(sorted_heads[0, at, :], sorted_heads[1, :n, :], NT) * scale
        s = jnp.where(causal(s.shape, i * qb, 0, 0), s, -jnp.inf)
        m = jnp.max(s, axis=1, keepdims=True)
        p = jnp.exp(s - m)
        l = jnp.sum(p, axis=1, keepdims=True)
        o = mm(p.astype(jnp.bfloat16), sorted_heads[2, :n, :]) / l
        o = o.astype(jnp.bfloat16)
        sorted_o[at, :] = o
        put(0, i, o)
        stat[0, at, :] = jnp.broadcast_to(m + jnp.log(l), (qb, hd))
        send_out(0, i)

    gather_end(1, dy_ref, dyr_ref)
    dy_copy = pltpu.make_async_copy(dyr_ref, dy_out, row_sem.at[1])
    dy_copy.start()
    wo_copy.wait()
    project(3, lambda at: mm(dyr_ref[...], wo_all[at, :], NT))
    width = dm // RS_TILES

    def rs_parts(tile, odd):
        onward, back = (left, right) if odd else (right, left)
        at = pl.ds(pl.multiple_of(tile * width, width), width)

        def mine(d):
            return (pl.ds(pl.multiple_of(d * rb, rb), rb), at)

        def copy(src, dst, send, recv, to):
            return pltpu.make_async_remote_copy(src, dst.at[tile], send.at[tile], recv.at[tile],
                                                device_id={"tp": to}, device_id_type=MESH)

        first = lambda: copy(part.at[mine(across)], r1, r1_send, r1_recv, onward)
        second = lambda: copy(s2.at[tile], r2, r2_send, r2_recv, onward)
        direct = lambda: copy(part.at[mine(back)], r3, r3_send, r3_recv, back)
        return at, mine, onward, first, second, direct

    def pairs_of_tiles(step):
        @pl.loop(0, RS_TILES // 2)
        def _(i):
            for odd in range(2):
                step(i * 2 + odd, odd)

    def reduce_first(tile, odd):
        at, _, _, first, _, _ = rs_parts(tile, odd)
        part[:, at] = mm(o_ref[...], wo_all[:, at])
        first().start()

    def reduce_direct(tile, odd):
        rs_parts(tile, odd)[5]().start()

    def reduce_second(tile, odd):
        _, mine, onward, first, second, _ = rs_parts(tile, odd)
        first().wait_recv()
        s2[tile] = r1[tile] + part[mine(onward)]
        second().start()

    def reduce_last(tile, odd):
        at, mine, _, first, second, direct = rs_parts(tile, odd)
        direct().wait_recv()
        second().wait_recv()
        y_ref[:, at] = (part[mine(me_t)] + r2[tile] + r3[tile]).astype(jnp.bfloat16)
        first().wait_send()
        second().wait_send()
        direct().wait_send()

    wait_out(0)
    pairs_of_tiles(reduce_first)
    pairs_of_tiles(reduce_direct)
    wait_in(3)
    for i in range(blocks):
        at = pl.ds(i * qb, qb)
        delta = jnp.sum(sorted_heads[3, at, :].astype(jnp.float32) * sorted_o[at, :].astype(jnp.float32), axis=1, keepdims=True)
        stat[1, at, :] = jnp.broadcast_to(delta, (qb, hd))
    for j in range(2):
        for i in range(total // hd):
            stat_t[j, :, i * hd:(i + 1) * hd] = stat[j, i * hd:(i + 1) * hd, :].T[:8]

    for i in walk:
        at, n = pl.ds(i * qb, qb), (i + 1) * qb
        s = mm(sorted_heads[0, at, :], sorted_heads[1, :n, :], NT) * scale
        p = jnp.where(causal(s.shape, i * qb, 0, 0), jnp.exp(s - stat[0, at, :1]), 0.0)
        dp = mm(sorted_heads[3, at, :], sorted_heads[2, :n, :], NT)
        ds = (p * (dp - stat[1, at, :1])).astype(jnp.bfloat16)
        put(1, i, (mm(ds, sorted_heads[1, :n, :]) * scale).astype(jnp.bfloat16))
        send_out(1, i)
    for i in walk:
        at, after = pl.ds(i * qb, qb), pl.ds(i * qb, total - i * qb)
        s = mm(sorted_heads[1, at, :], sorted_heads[0, after, :], NT) * scale
        p = jnp.where(causal(s.shape, 0, 0, 1), jnp.exp(s - stat_t[0, :1, after]), 0.0)
        dp = mm(sorted_heads[2, at, :], sorted_heads[3, after, :], NT)
        ds = (p * (dp - stat_t[1, :1, after])).astype(jnp.bfloat16)
        put(3, i, mm(p.astype(jnp.bfloat16), sorted_heads[3, after, :]).astype(jnp.bfloat16))
        send_out(3, i)
        put(2, i, (mm(ds, sorted_heads[0, after, :]) * scale).astype(jnp.bfloat16))
        send_out(2, i)

    pairs_of_tiles(reduce_second)


    def dx_copy(tile, odd):
        spot = (pl.ds(pl.multiple_of(across * rb, rb), rb), pl.ds(pl.multiple_of((tile + odd * RS_TILES // 2) * width, width), width))
        return pltpu.make_async_remote_copy(dx_part.at[spot], r4.at[odd, tile], r4_send.at[odd, tile], r4_recv.at[odd, tile],
                                            device_id={"tp": left if odd else right}, device_id_type=MESH)

    def block_of(d, at):
        return dx_part[pl.ds(pl.multiple_of(d * rb, rb), rb), at]

    def dx_term(t, w, at):
        return mm(outs[t][...], wall[w, at, :], NT)

    for t, w in ((1, 0), (3, 2)):
        wait_out(t)

        @pl.loop(0, RS_TILES)
        def _(i):
            at = pl.ds(pl.multiple_of(i * width, width), width)
            term = dx_term(t, w, at)
            dx_part[:, at] = term if t == 1 else dx_part[:, at] + term

    wait_out(2)

    @pl.loop(0, RS_TILES // 2)
    def _(i):
        for odd, (back_ref, back) in enumerate(((back_l, left), (back_r, right))):
            at = pl.ds(pl.multiple_of((i + odd * RS_TILES // 2) * width, width), width)
            dx_part[:, at] += dx_term(2, 1, at)
            dx_copy(i, odd).start()
            own_ref[:, at] = block_of(me_t, at)
            back_ref[:, pl.ds(pl.multiple_of(i * width, width), width)] = block_of(back, at)

    pairs_of_tiles(reduce_last)

    @pl.loop(0, RS_TILES // 2)
    def _(i):
        for odd, (on_ref, onward) in enumerate(((on_r, right), (on_l, left))):
            at = pl.ds(pl.multiple_of((i + odd * RS_TILES // 2) * width, width), width)
            dx_copy(i, odd).wait_recv()
            on_ref[:, pl.ds(pl.multiple_of(i * width, width), width)] = r4[odd, i] + block_of(onward, at)
            dx_copy(i, odd).wait_send()

    x_copy.wait()
    dy_copy.wait()
    for t in range(4):
        for sem in (in_send, out_send):
            pltpu.make_async_copy(others, others, sem.at[t]).wait()
    for which, src, dst in ((0, x_ref, xr_ref), (1, dy_ref, dyr_ref)):
        for idx, col_half, to in ((0, 0, right), (1, 1, left), (2, 1, right), (3, 0, left)):
            gather_copy(src, dst, which, idx, me_t, col_half, to).wait_send()
        gather_copy(dst, dst, which, 4, left, 0, right).wait_send()
        gather_copy(dst, dst, which, 5, right, 1, left).wait_send()


def attention_call(tp, cp, x_blk, dy_blk, wq, wk, wv, wo):
    rb, dm = x_blk.shape
    rows = rb * tp
    hc, _ = wo.shape
    hd = hc // cp
    total = rows * cp
    bf, f32 = jnp.bfloat16, jnp.float32
    chunk = dm // CHUNKS
    width = dm // RS_TILES
    vmem, hbm = pl.BlockSpec(memory_space=pltpu.VMEM), pl.BlockSpec(memory_space=pl.ANY)
    out = lambda r, c: jax.ShapeDtypeStruct((r, c), bf)
    wide = lambda c: jax.ShapeDtypeStruct((rb, c), f32)
    dma = pltpu.SemaphoreType.DMA
    return pl.pallas_call(
        functools.partial(attention_kernel, tp, cp),
        out_shape=(out(rb, dm), wide(dm), *[wide(dm // 2)] * 4, out(rows, dm), out(rows, dm), out(rows, hc), out(rows, hc), out(rows, hc), out(rows, hc)),
        in_specs=[hbm] * 6,
        out_specs=[vmem] * 6 + [hbm] * 2 + [vmem] * 4,
        scratch_shapes=[
            pltpu.VMEM((rb, dm), bf), pltpu.VMEM((rb, dm), bf), pltpu.VMEM((rows, dm), bf), pltpu.VMEM((rows, dm), bf),
            pltpu.VMEM((SLOTS, chunk * cp, hd), bf), pltpu.VMEM((STRIPS, chunk // STRIPS * max(cp, PITCH), hd), f32),
            pltpu.VMEM((3, dm, hc), bf), pltpu.VMEM((hc, dm), bf),
            pltpu.VMEM((4, rows, hc), bf), pltpu.VMEM((4, total, hd), bf),
            pltpu.VMEM((4, total, hd), bf), pltpu.VMEM((total, hd), bf), pltpu.VMEM((4, total, hd), bf),
            pltpu.VMEM((2, total, hd), f32), pltpu.VMEM((2, 8, total), f32),
            pltpu.VMEM((rows, dm), f32), pltpu.VMEM((rows, dm), f32),
            pltpu.VMEM((RS_TILES, rb, width), f32), pltpu.VMEM((RS_TILES, rb, width), f32),
            pltpu.VMEM((RS_TILES, rb, width), f32), pltpu.VMEM((RS_TILES, rb, width), f32),
            pltpu.VMEM((2, RS_TILES // 2, rb, width), f32),
            dma((SLOTS,)), dma, dma((2,)), dma((2,)), dma((2, 6)), dma((2, 6)), dma((4,)), dma((4,)), dma((4,)), dma((4,)),
            *[dma((RS_TILES,))] * 6, *[dma((2, RS_TILES // 2))] * 2,
        ],
        compiler_params=pltpu.CompilerParams(collective_id=0, has_side_effects=True, vmem_limit_bytes=VMEM_BYTES),
    )(x_blk, dy_blk, wq, wk, wv, wo)


def grad_kernel(n_heads, x_hbm, dy_hbm, o_hbm, dq_hbm, dk_hbm, dv_hbm, y_hbm, gq_ref, gk_ref, gv_ref, go_ref, y_out,
                x_ref, dy_ref, o_ref, dq_ref, dk_ref, dv_ref, y_ref, wide, grads, out_grad, in_sem, out_sem):
    rows, dm = x_ref.shape
    hd = wide.shape[-1]
    tiles = grads.shape[1]
    m_tile = dm // tiles
    pitch = wide.shape[1] // m_tile
    loads = [pltpu.make_async_copy(src, dst, in_sem.at[i]) for i, (src, dst) in enumerate(
        ((dq_hbm, dq_ref), (x_hbm, x_ref), (dk_hbm, dk_ref), (dv_hbm, dv_ref), (o_hbm, o_ref), (dy_hbm, dy_ref), (y_hbm, y_ref)))]
    for load in loads:
        load.start()
    for load in loads[:4]:
        load.wait()

    @pl.loop(0, tiles)
    def _(i):
        at = pl.ds(pl.multiple_of(i * m_tile, m_tile), m_tile)
        tall = pl.ds(pl.multiple_of(i * m_tile * n_heads, m_tile * n_heads), m_tile * n_heads)
        x_t = x_ref[:, at].T
        for t, (d_ref, g_ref) in enumerate(((dq_ref, gq_ref), (dk_ref, gk_ref), (dv_ref, gv_ref))):
            for h in range(0, n_heads, 2):
                grad = mm(x_t, d_ref[:, h * hd:(h + 2) * hd])
                for e in range(2):
                    wide[t, pl.ds(h + e, m_tile, stride=pitch), :] = grad[:, e * hd:(e + 1) * hd]
            for r in range(0, m_tile, 2):
                pair = jnp.concatenate([wide[t, (r + e) * pitch:(r + e) * pitch + n_heads, :] for e in range(2)], axis=0)
                grads[t, i, r * n_heads:(r + 2) * n_heads, :] = pair.astype(jnp.bfloat16)
            pltpu.make_async_copy(grads.at[t, i], g_ref.at[tall], out_sem.at[t]).start()

    for load in loads[4:]:
        load.wait()
    y_out_copy = pltpu.make_async_copy(y_ref, y_out, out_sem.at[4])
    y_out_copy.start()

    o_rows, o_cols = out_grad.shape[1:]
    across = dm // o_cols

    @pl.loop(0, out_grad.shape[0])
    def _(i):
        r, c = pl.multiple_of(i // across * o_rows, o_rows), pl.multiple_of(i % across * o_cols, o_cols)
        out_grad[i] = mm(o_ref[:, pl.ds(r, o_rows)], dy_ref[:, pl.ds(c, o_cols)], TN).astype(jnp.bfloat16)
        pltpu.make_async_copy(out_grad.at[i], go_ref.at[pl.ds(r, o_rows), pl.ds(c, o_cols)], out_sem.at[3]).start()

    y_out_copy.wait()
    for t, g_ref in enumerate((gq_ref, gk_ref, gv_ref, go_ref)):
        pltpu.make_async_copy(g_ref, g_ref, out_sem.at[t]).wait()


def grad_call(n_heads, x_rows, dy_rows, o_flat, dq, dk, dv, y_blk):
    rows, dm = x_rows.shape
    hc = o_flat.shape[1]
    hd = hc // n_heads
    tiles = n_heads
    bf, f32 = jnp.bfloat16, jnp.float32
    hbm = pl.BlockSpec(memory_space=pl.ANY)
    inputs = (x_rows, dy_rows, o_flat, dq, dk, dv, y_blk)
    o_rows, o_cols = hc // 2, dm // 4
    return pl.pallas_call(
        functools.partial(grad_kernel, n_heads),
        out_shape=[jax.ShapeDtypeStruct((dm * n_heads, hd), bf)] * 3 + [jax.ShapeDtypeStruct((hc, dm), bf), jax.ShapeDtypeStruct(y_blk.shape, bf)],
        in_specs=[hbm] * 7,
        out_specs=[hbm] * 5,
        scratch_shapes=[*[pltpu.VMEM(a.shape, bf) for a in inputs],
                        pltpu.VMEM((3, dm // tiles * max(n_heads, PITCH), hd), f32), pltpu.VMEM((3, tiles, dm // tiles * n_heads, hd), bf),
                        pltpu.VMEM((8, o_rows, o_cols), bf), pltpu.SemaphoreType.DMA((7,)), pltpu.SemaphoreType.DMA((5,))],
        compiler_params=pltpu.CompilerParams(vmem_limit_bytes=VMEM_BYTES),
        cost_estimate=pl.CostEstimate(flops=8 * rows * dm * hc, bytes_accessed=8 * dm * hc + 8 * rows * dm, transcendentals=0),
    )(*inputs)


def add_kernel(own, direct_a, last_a, direct_b, last_b, dx_ref):
    cols = direct_a.shape[1]
    dx_ref[:, :cols] = (own[:, :cols] + direct_a[...] + last_a[...]).astype(jnp.bfloat16)
    dx_ref[:, cols:] = (own[:, cols:] + direct_b[...] + last_b[...]).astype(jnp.bfloat16)


def solution(mesh):
    tp, cp = mesh.shape["tp"], mesh.shape["cp"]

    def device_fn(x_blk, w_query, w_key, w_value, w_out, dy_blk):
        dm, n_heads, hd = w_query.shape
        if tp != 4 or n_heads != cp or w_key.shape != w_query.shape:
            raise ValueError("unsupported split")
        tall = lambda w: w.reshape(dm * n_heads, hd)
        y_blk, own, back_l, back_r, on_r, on_l, x_rows, dy_rows, o_flat, dq, dk, dv = attention_call(
            tp, cp, x_blk, dy_blk, tall(w_query), tall(w_key), tall(w_value), w_out.reshape(n_heads * hd, dm))
        to_right = lambda a: lax.ppermute(a, "tp", [(i, (i + 1) % tp) for i in range(tp)])
        to_left = lambda a: lax.ppermute(a, "tp", [(i, (i - 1) % tp) for i in range(tp)])
        last_a, last_b, direct_a, direct_b = to_right(on_r), to_left(on_l), to_left(back_l), to_right(back_r)
        gq, gk, gv, go, y_blk = grad_call(n_heads, x_rows, dy_rows, o_flat, dq, dk, dv, y_blk)
        vmem = pl.BlockSpec(memory_space=pltpu.VMEM)
        dx_blk = pl.pallas_call(add_kernel, out_shape=jax.ShapeDtypeStruct(own.shape, jnp.bfloat16), in_specs=[vmem] * 5, out_specs=vmem)(
            own, direct_a, last_a, direct_b, last_b)
        split = lambda g: g.reshape(1, dm, n_heads, hd)
        return y_blk, dx_blk, split(gq), split(gk), split(gv), go.reshape(1, n_heads, hd, dm)

    return jax.shard_map(device_fn, mesh=mesh,
                         in_specs=(ROW_SPEC, HEAD_SPEC, HEAD_SPEC, HEAD_SPEC, OUT_W_SPEC, ROW_SPEC),
                         out_specs=(ROW_SPEC, ROW_SPEC, GRAD_SPEC, GRAD_SPEC, GRAD_SPEC, GRAD_OUT_SPEC),
                         check_vma=False)
```
